32 devices in a mesh: dp: 8 (over z, core), tensor: 4 (over y, x).
Axes of the slice: x: 2, y: 2, z: 4, core: 2. Of those that a mesh axis runs over, the one named last changes fastest.
Arguments:
- hidden_in: bfloat16 [32, 128, 896], P('dp', 'tensor'), may hold values from -6 to 6
- targets: int32 [32, 128], P('dp', 'tensor'), may hold values from 0 to 98303
- doc_blocks: int32 [16], replicated, may hold values from 1 to 4, as said below
- ref_milli: int32 [16], replicated, may hold values from 8000 to 13999
- attn_gain: float32 [2, 896], replicated, may hold values from 0.3 to 3
- mlp_gain: float32 [2, 896], replicated, may hold values from 0.3 to 3
- final_gain: float32 [896], replicated, may hold values from 0.3 to 3
- w_query: bfloat16 [2, 896, 896], replicated, may hold values from -8.1 to 8.1
- w_key: bfloat16 [2, 896, 128], replicated, may hold values from -0.1875 to 0.1875
- w_value: bfloat16 [2, 896, 128], replicated, may hold values from -0.1875 to 0.1875
- w_out: bfloat16 [2, 896, 896], replicated, may hold values from -0.1875 to 0.1875
- w_gate: bfloat16 [2, 896, 4864], P(None, None, 'tensor'), may hold values from -0.1875 to 0.1875
- w_up: bfloat16 [2, 896, 4864], P(None, None, 'tensor'), may hold values from -0.1875 to 0.1875
- w_down: bfloat16 [2, 4864, 896], P(None, 'tensor'), may hold values from -0.078125 to 0.078125
- w_head: bfloat16 [896, 98304], P(None, ('dp', 'tensor')), may hold values from -41 to 41
Outputs:
- token_loss: float32 [32, 128], P('dp', 'tensor')
- scores: float32 [16], replicated
The draws below stay inside these ranges and needn't reach their ends.
Inputs may be any that keep to these rules, and one draw needn't show every extreme that they name: `doc_blocks`: lengths of the documents in blocks, in pack order; they sum to 32.
All inputs are finite; a program needn't handle non-finite values.
Results may differ from the reference program's by a relative error of at most 0.035.
Values may be sent and summed in bfloat16 or wider, within the bound.
No kernel may reach another device: no remote copies, remote signals or barrier semaphores. Data moves between devices by JAX's collectives and lax.ppermute only.
A program may use at most 192 MiB of HBM per device.

```python
import math
import jax
import jax.numpy as jnp
import numpy as np
from jax import lax

D = 896
HEADS = 14
KV_HEADS = 2
HEAD_DIM = 64
FF = 4864
V = 98304
LAYERS = 2
BLK = 128
MAXB = 4
BLK_DEV = 4
NBLK = 32
NDOC = 16


def draw_doc_blocks(key, part):

    def step(start, index):
        left_docs = NDOC - index
        remain = NBLK - start
        lowest = jnp.maximum(1, remain - (left_docs - 1) * MAXB).astype(jnp.int32)
        highest = jnp.minimum(MAXB, remain - (left_docs - 1)).astype(jnp.int32)
        length = jax.random.randint(jax.random.fold_in(key, index), (), lowest, highest + 1, dtype=jnp.int32)
        covers = (start <= BLK_DEV - 1) & (start + length > BLK_DEV - 1)
        forced = jnp.where(start == BLK_DEV - MAXB, MAXB - 1, MAXB).astype(jnp.int32)
        length = jnp.where(covers, forced, length).astype(jnp.int32)
        return ((start + length).astype(jnp.int32), length)
    unused, lengths = lax.scan(step, jnp.int32(0), jnp.arange(NDOC, dtype=jnp.int32))
    return lengths.astype(jnp.int32)


def draw_w_query(key, part):
    base = jnp.clip(jax.random.normal(key, (LAYERS, D, D), jnp.float32), -6.0, 6.0) * D ** (-0.5)
    return base.astype(jnp.bfloat16)


def draw_w_head(key, part):
    base = jnp.clip(jax.random.normal(key, (D, V), jnp.float32), -6.0, 6.0) * (2.5 / math.sqrt(D))
    return base.astype(jnp.bfloat16)


def plant(drawn, key, least, top_value):
    index_at = [jax.random.randint(jax.random.fold_in(key, axis), (), 0, length) for axis, length in enumerate(drawn.shape)]
    main_axis = drawn.shape.index(max(drawn.shape))
    beside = index_at[:main_axis] + [(index_at[main_axis] + 1) % drawn.shape[main_axis]] + index_at[main_axis + 1:]
    return drawn.at[tuple(index_at)].set(least).at[tuple(beside)].set(top_value)


def level_of(rng, extent, pieces, smallest, high):
    def one(axis_at, parts):
        draws = jax.random.uniform(jax.random.fold_in(jax.random.fold_in(rng, 6), axis_at), (parts,), jnp.float32, smallest / len(pieces), high / len(pieces))
        return jnp.repeat(jnp.exp(draws), extent[axis_at] // parts).reshape((-1,) + (1,) * (len(extent) - axis_at - 1))

    loudness = one(*pieces[0])
    for cut in pieces[1:]:
        loudness = loudness * one(*cut)
    return loudness


def wide_ids(stream_key, shape, number_of, skew):
    weights = [min(1 << octave, number_of + 1 - (1 << octave)) * (1 << 20) // math.isqrt((1 << octave) ** skew) + 1 for octave in range((number_of + 1).bit_length()) if 1 << octave <= number_of]
    width = 1 + sum(weights) // (1 << 30)
    grid = np.cumsum(np.array([max(1, weight // width) for weight in weights]))
    ticket = jax.random.randint(jax.random.fold_in(stream_key, 1), shape, 0, int(grid[len(weights) - 1]))
    start = jnp.left_shift(1, jnp.searchsorted(jnp.asarray(grid, jnp.int32), ticket, side="right").astype(jnp.int32))
    rank = start - 1 + jax.random.randint(jax.random.fold_in(stream_key, 4), shape, 0, 1 << 30) % jnp.minimum(start, number_of + 1 - start)
    return jax.random.permutation(jax.random.fold_in(stream_key, 2), number_of)[rank].astype(jnp.int32)


def bell_draw(rng, dims, width, reach, cuts=(), kind=jnp.bfloat16):
    entries = jax.random.normal(rng, dims, jnp.float32) * width
    if len(cuts) > 0:
        entries = level_of(rng, dims, cuts, -0.22, 0.18) * entries
    return jnp.clip(entries, min=-reach, max=reach).astype(kind)


def setup_inputs(seed: int = 0) -> dict:
    streams_of = jax.random.split(jax.random.key(seed), 16)
    return {
        "hidden_in": bell_draw(streams_of[0], (NBLK, BLK, D), 1.0, 6.0, ((0, 8), (1, 4))),
        "targets": plant(wide_ids(streams_of[1], (NBLK, BLK), V, 2), jax.random.fold_in(streams_of[1], 3), 0, V - 1).astype(jnp.int32),
        "doc_blocks": draw_doc_blocks(jax.random.fold_in(streams_of[15], 71), 0),
        "ref_milli": plant(jax.random.randint(streams_of[3], (NDOC,), 8000, 14000), jax.random.fold_in(streams_of[3], 1), 8000, 13999).astype(jnp.int32),
        "attn_gain": jnp.clip(jnp.exp(jax.random.uniform(streams_of[4], (LAYERS, D), jnp.float32, math.log(0.3), math.log(3.0))), 0.3, 3.0),
        "mlp_gain": jnp.clip(jnp.exp(jax.random.uniform(streams_of[5], (LAYERS, D), jnp.float32, math.log(0.3), math.log(3.0))), 0.3, 3.0),
        "final_gain": jnp.clip(jnp.exp(jax.random.uniform(streams_of[6], (D,), jnp.float32, math.log(0.3), math.log(3.0))), 0.3, 3.0),
        "w_query": draw_w_query(jax.random.fold_in(streams_of[15], 71), 0),
        "w_key": bell_draw(streams_of[8], (LAYERS, D, KV_HEADS * HEAD_DIM), D ** -0.5, 0.1875),
        "w_value": bell_draw(streams_of[9], (LAYERS, D, KV_HEADS * HEAD_DIM), D ** -0.5, 0.1875),
        "w_out": bell_draw(streams_of[10], (LAYERS, D, D), D ** -0.5, 0.1875),
        "w_gate": bell_draw(streams_of[11], (LAYERS, D, FF), D ** -0.5, 0.1875, ((2, 4),)),
        "w_up": bell_draw(streams_of[12], (LAYERS, D, FF), D ** -0.5, 0.1875, ((2, 4),)),
        "w_down": bell_draw(streams_of[13], (LAYERS, FF, D), FF ** -0.5, 0.078125, ((1, 4),)),
        "w_head": draw_w_head(jax.random.fold_in(streams_of[15], 71), 0),
    }


def doc_table(doc_blocks, nblk):
    ends = jnp.cumsum(doc_blocks).astype(jnp.int32)
    starts = (ends - doc_blocks).astype(jnp.int32)
    ids = jnp.arange(nblk, dtype=jnp.int32)
    owner = lax.optimization_barrier(jnp.sum((starts[None, :] <= ids[:, None]).astype(jnp.int32), axis=1)).astype(jnp.int32) - 1
    hit = owner[:, None] == jnp.arange(doc_blocks.shape[0], dtype=jnp.int32)[None, :]
    first = lax.optimization_barrier(jnp.sum(jnp.where(hit, starts[None, :], 0), axis=1)).astype(jnp.int32)
    return (owner, (ids - first).astype(jnp.int32))

def norm_rows(h, gain):
    return h * lax.rsqrt(lax.optimization_barrier(jnp.mean(h * h, axis=-1, keepdims=True)) + 1e-06) * gain

def rotate(x, pos):
    half = x.shape[-1] // 2
    freq = jnp.exp(jnp.arange(half, dtype=jnp.float32) * (-2.0 * math.log(1000000.0) / x.shape[-1]))
    angle = pos.astype(jnp.float32)[..., None, None] * freq
    cosine = jnp.cos(angle)
    sine = jnp.sin(angle)
    first = x[..., :half]
    second = x[..., half:]
    return jnp.concatenate([first * cosine - second * sine, second * cosine + first * sine], axis=-1)

def attend(query, keys, values, qdoc, qpos, kdoc, kpos):
    count, nheads, hdim = query.shape
    kvh = keys.shape[-1] // hdim
    q_five = query.reshape(count, kvh, nheads // kvh, hdim).astype(jnp.float32)
    k_three = keys.reshape(-1, kvh, hdim).astype(jnp.float32)
    v_three = values.reshape(-1, kvh, hdim).astype(jnp.float32)
    logits = jnp.einsum('qcgd,kcd->cgqk', q_five, k_three) * hdim ** (-0.5)
    allowed = (qdoc[:, None] == kdoc[None, :]) & (kpos[None, :] <= qpos[:, None]) & (kdoc[None, :] >= 0)
    logits = jnp.where(allowed, logits, -1e+30)
    peak = lax.optimization_barrier(jnp.max(logits, axis=-1, keepdims=True))
    expo = jnp.exp(logits - peak)
    weights = (expo / lax.optimization_barrier(jnp.sum(expo, axis=-1, keepdims=True))).astype(jnp.bfloat16)
    context = jnp.einsum('cgqk,kcd->qcgd', weights.astype(jnp.float32), v_three)
    return context.reshape(count, nheads * hdim).astype(jnp.bfloat16)

def reference(hidden_in, targets, doc_blocks, ref_milli, attn_gain, mlp_gain, final_gain, w_query, w_key, w_value, w_out, w_gate, w_up, w_down, w_head):
    nblk = hidden_in.shape[0]
    total = nblk * BLK
    owner, offset = doc_table(doc_blocks, nblk)
    tok_doc = jnp.repeat(owner, BLK)
    tok_pos = (offset[:, None] * BLK + jnp.arange(BLK, dtype=jnp.int32)[None, :]).reshape(-1)
    pad = (MAXB - 1) * BLK
    doc_pad = jnp.concatenate([jnp.full((pad,), -1, jnp.int32), tok_doc])
    pos_pad = jnp.concatenate([jnp.zeros((pad,), jnp.int32), tok_pos])
    h = hidden_in.reshape(total, D).astype(jnp.float32)
    for layer in range(LAYERS):
        a = norm_rows(h, attn_gain[layer]).astype(jnp.bfloat16)
        q = jnp.dot(a, w_query[layer], preferred_element_type=jnp.float32).reshape(total, HEADS, HEAD_DIM)
        q = rotate(q, tok_pos).astype(jnp.bfloat16)
        k = jnp.dot(a, w_key[layer], preferred_element_type=jnp.float32).reshape(total, KV_HEADS, HEAD_DIM)
        k = rotate(k, tok_pos).astype(jnp.bfloat16).reshape(total, KV_HEADS * HEAD_DIM)
        v = jnp.dot(a, w_value[layer], preferred_element_type=jnp.float32).astype(jnp.bfloat16)
        k_pad = jnp.concatenate([jnp.zeros((pad, KV_HEADS * HEAD_DIM), jnp.bfloat16), k])
        v_pad = jnp.concatenate([jnp.zeros((pad, KV_HEADS * HEAD_DIM), jnp.bfloat16), v])

        def one_block(index):
            lead = (index * BLK).astype(jnp.int32)
            query = lax.dynamic_slice_in_dim(q, lead, BLK, 0)
            qdoc = lax.dynamic_slice_in_dim(tok_doc, lead, BLK, 0)
            qpos = lax.dynamic_slice_in_dim(tok_pos, lead, BLK, 0)
            keys = lax.dynamic_slice_in_dim(k_pad, lead, MAXB * BLK, 0)
            values = lax.dynamic_slice_in_dim(v_pad, lead, MAXB * BLK, 0)
            kdoc = lax.dynamic_slice_in_dim(doc_pad, lead, MAXB * BLK, 0)
            kpos = lax.dynamic_slice_in_dim(pos_pad, lead, MAXB * BLK, 0)
            return attend(query, keys, values, qdoc, qpos, kdoc, kpos)
        context = lax.map(one_block, jnp.arange(nblk, dtype=jnp.int32)).reshape(total, D)
        h = h + jnp.dot(context, w_out[layer], preferred_element_type=jnp.float32)
        b = norm_rows(h, mlp_gain[layer]).astype(jnp.bfloat16)
        gate = jnp.dot(b, w_gate[layer], preferred_element_type=jnp.float32)
        upper = jnp.dot(b, w_up[layer], preferred_element_type=jnp.float32)
        middle = (jax.nn.silu(gate) * upper).astype(jnp.bfloat16)
        h = h + jnp.dot(middle, w_down[layer], preferred_element_type=jnp.float32)
    final = norm_rows(h, final_gain).astype(jnp.bfloat16)

    def head_block(index):
        lead = (index * BLK).astype(jnp.int32)
        rows = lax.dynamic_slice_in_dim(final, lead, BLK, 0)
        wanted = lax.dynamic_slice_in_dim(targets.reshape(-1), lead, BLK, 0)
        logits = jnp.dot(rows, w_head, preferred_element_type=jnp.float32)
        peak = lax.optimization_barrier(jnp.max(logits, axis=1))
        spread = jnp.log(lax.optimization_barrier(jnp.sum(jnp.exp(logits - peak[:, None]), axis=1))) + peak
        picked = jnp.take_along_axis(logits, wanted[:, None].astype(jnp.int32), axis=1)[:, 0]
        return spread - picked
    token_loss = lax.map(head_block, jnp.arange(nblk, dtype=jnp.int32))
    block_sum = lax.optimization_barrier(jnp.sum(token_loss, axis=1))
    hit = owner[:, None] == jnp.arange(doc_blocks.shape[0], dtype=jnp.int32)[None, :]
    doc_total = lax.optimization_barrier(jnp.sum(jnp.where(hit, block_sum[:, None], 0.0), axis=0))
    scores = ref_milli.astype(jnp.float32) * 0.001 - doc_total / (doc_blocks * BLK).astype(jnp.float32)
    return (token_loss, scores)
```

```python
import math

import jax
import jax.numpy as jnp
from jax import lax
from jax.experimental import pallas as pl
from jax.experimental.pallas import tpu as pltpu
from jax.sharding import Mesh
from jax.sharding import PartitionSpec as P

HEAD_DIM = 64
MAXB = 4
LANES = 128
NEG = -1e30
BF16 = jnp.bfloat16
F32 = jnp.float32
DP = ("zp", "zq", "core")
ALL = ("zp", "zq", "core", "tensor")
MIB = 1024 * 1024


def doc_table(doc_blocks, nblk):
    ends = jnp.cumsum(doc_blocks)
    starts = ends - doc_blocks
    ids = jnp.arange(nblk, dtype=jnp.int32)
    owner = jnp.sum((starts[None, :] <= ids[:, None]).astype(jnp.int32), axis=1) - 1
    hit = owner[:, None] == jnp.arange(doc_blocks.shape[0], dtype=jnp.int32)[None, :]
    first = jnp.sum(jnp.where(hit, starts[None, :], 0), axis=1)
    return (owner, ids - first)


def lookup(block_ids, table, nblk):
    hit = block_ids[:, None] == jnp.arange(nblk, dtype=jnp.int32)[None, :]
    found = jnp.sum(jnp.where(hit, table[None, :], 0), axis=1)
    inside = (block_ids >= 0) & (block_ids < nblk)
    return (found, inside)


def norm_rows(h, gain):
    scaled = h * lax.rsqrt(jnp.mean(h * h, axis=-1, keepdims=True) + 1e-06)
    return (scaled.reshape(-1, 8, h.shape[1]) * gain[None]).reshape(h.shape)


def tall(gain):
    shape = gain.shape[:-1] + (8, gain.shape[-1])
    return jnp.broadcast_to(gain[..., None, :], shape)


def dot(x, y):
    return jnp.dot(x, y, preferred_element_type=F32)


def dot_t(x, y):
    return lax.dot_general(x, y, (((1,), (1,)), ((), ())), preferred_element_type=F32)


def whole(shape):
    return pl.BlockSpec(shape, lambda *_: (0,) * len(shape))


def layer_of(array, layer):
    shape = array.shape[1:]
    return pl.BlockSpec((None,) + shape, lambda *_: (layer,) + (0,) * len(shape))


def cost(flops, moved):
    return pl.CostEstimate(flops=int(flops), bytes_accessed=int(moved), transcendentals=0)


def params(mib):
    return pltpu.CompilerParams(vmem_limit_bytes=mib * MIB)


def rotate_lanes(x, cosine, sine):
    lane = lax.broadcasted_iota(jnp.int32, (x.shape[0], LANES), 1)
    lower = lane % HEAD_DIM < HEAD_DIM // 2
    pieces = []
    for at in range(0, x.shape[1], LANES):
        part = x[:, at : at + LANES]
        other = jnp.where(
            lower,
            pltpu.roll(part, LANES - HEAD_DIM // 2, 1),
            pltpu.roll(part, HEAD_DIM // 2, 1),
        )
        pieces.append(part * cosine + other * sine)
    return pieces


def add_parts(h, refs):
    for ref in refs:
        h = h + ref[...].astype(F32)
    return h


def key_value(h, parts, gains, w_key, w_value, cosine, sine, layer):
    count, width = h.shape
    kvw = w_key.shape[-1]

    def body(*refs):
        h_ref, given, refs = refs[0], refs[1 : 1 + len(parts)], refs[1 + len(parts) :]
        value = add_parts(h_ref[...].astype(F32), given)
        gain_ref, wk_ref, wv_ref, cos_ref, sin_ref, h_out, a_out, kv_out = refs
        h_out[...] = value
        a = norm_rows(value, gain_ref[...]).astype(BF16)
        a_out[...] = a
        keys = rotate_lanes(dot(a, wk_ref[...]), cos_ref[...], sin_ref[...])
        for at, piece in enumerate(keys):
            kv_out[:, at * LANES : (at + 1) * LANES] = piece.astype(BF16)
        kv_out[:, kvw:] = dot(a, wv_ref[...]).astype(BF16)

    args = [h] + parts + [gains, w_key, w_value, cosine, sine]
    specs = [whole(x.shape) for x in args]
    specs[-5] = layer_of(gains, layer)
    specs[-4] = layer_of(w_key, layer)
    specs[-3] = layer_of(w_value, layer)
    outs = (
        jax.ShapeDtypeStruct((count, width), F32),
        jax.ShapeDtypeStruct((count, width), BF16),
        jax.ShapeDtypeStruct((count, 2 * kvw), BF16),
    )
    return pl.pallas_call(
        body,
        grid=(1,),
        out_shape=outs,
        in_specs=specs,
        out_specs=[whole(o.shape) for o in outs],
        compiler_params=params(12),
        cost_estimate=cost(2.0 * count * width * 2 * kvw, 0),
        name="key_value",
    )(*args)


def queries(a, w_query, cosine, sine, layer):
    count = a.shape[0]
    out = w_query.shape[-1]

    def body(a_ref, w_ref, cos_ref, sin_ref, q_out):
        q = rotate_lanes(dot(a_ref[...], w_ref[...]), cos_ref[...], sin_ref[...])
        for at, piece in enumerate(q):
            q_out[:, at * LANES : (at + 1) * LANES] = piece.astype(BF16)

    shape = (count, out)
    return pl.pallas_call(
        body,
        grid=(1,),
        out_shape=jax.ShapeDtypeStruct(shape, BF16),
        in_specs=[
            whole(a.shape),
            layer_of(w_query, layer),
            whole(cosine.shape),
            whole(sine.shape),
        ],
        out_specs=whole(shape),
        compiler_params=params(10),
        cost_estimate=cost(2.0 * count * out * out, 0),
        name="queries",
    )(a, w_query, cosine, sine)


def attention(q, kv, bias, h, w_out, gains, layer):
    blocks, rows, span = bias.shape
    count, qw = q.shape
    width = h.shape[1]
    kvw = kv.shape[1] // 2
    kvh = kvw // HEAD_DIM
    heads = qw // HEAD_DIM
    group = heads // kvh
    pairs = heads // 2
    block_len = span // MAXB
    assert kvw == LANES and kvh == 2

    def body(q_ref, kv_ref, bias_ref, h_ref, wo_ref, gain_ref, h_out, b_out, score, ctx):
        low = lax.broadcasted_iota(jnp.int32, (kv_ref.shape[0], LANES), 1) < HEAD_DIM

        def variants(x, other):
            turned = pltpu.roll(x, HEAD_DIM, 1)
            return {
                (0, 0): jnp.where(low, x, other).astype(BF16),
                (1, 1): jnp.where(low, other, x).astype(BF16),
                (0, 1): jnp.where(low, turned, other).astype(BF16),
                (1, 0): jnp.where(low, other, turned).astype(BF16),
            }

        keys = variants(kv_ref[:, :kvw].astype(F32), 0.0)
        values = variants(kv_ref[:, kvw:].astype(F32), 1.0)
        work = []
        at = 0
        for i in range(blocks):
            for half in range(2):
                for c in range(kvh):
                    mine = [j for j in range(pairs) if (2 * j + half) // group == c]
                    if mine:
                        work.append((i, half, c, mine, at))
                        at += len(mine) * rows
        for i, half, c, mine, at in work:
            window = slice(i * block_len, i * block_len + span)
            stack = [q_ref[i * rows : (i + 1) * rows, j * LANES : (j + 1) * LANES] for j in mine]
            found = dot_t(jnp.concatenate(stack, axis=0), keys[(half, c)][window])
            for n in range(len(mine)):
                piece = found[n * rows : (n + 1) * rows] * HEAD_DIM ** (-0.5) + bias_ref[i]
                score[at + n * rows : at + (n + 1) * rows] = piece
        halves = {}
        for i, half, c, mine, at in work:
            window = slice(i * block_len, i * block_len + span)
            piece = score[at : at + len(mine) * rows]
            expo = jnp.exp(piece - jnp.max(piece, axis=-1, keepdims=True)).astype(BF16)
            got = dot(expo, values[(half, c)][window])
            got = got / pltpu.roll(got, HEAD_DIM, 1)
            for n, j in enumerate(mine):
                halves[(i, j, half)] = got[n * rows : (n + 1) * rows]
        first = low[:rows]
        for i in range(blocks):
            for j in range(pairs):
                ctx[i * rows : (i + 1) * rows, j * LANES : (j + 1) * LANES] = jnp.where(
                    first, halves[(i, j, 0)], halves[(i, j, 1)]
                )
        value = h_ref[...] + dot(ctx[...].astype(BF16), wo_ref[...])
        h_out[...] = value
        b_out[...] = norm_rows(value, gain_ref[...]).astype(BF16)

    args = (q, kv, bias, h, w_out, gains)
    specs = [whole(x.shape) for x in args]
    specs[4] = layer_of(w_out, layer)
    specs[5] = layer_of(gains, layer)
    outs = (
        jax.ShapeDtypeStruct((count, width), F32),
        jax.ShapeDtypeStruct((count, width), BF16),
    )
    return pl.pallas_call(
        body,
        grid=(1,),
        out_shape=outs,
        in_specs=specs,
        out_specs=[whole(o.shape) for o in outs],
        scratch_shapes=[
            pltpu.VMEM((blocks * heads * rows, span), F32),
            pltpu.VMEM((count, qw), F32),
        ],
        compiler_params=params(20),
        cost_estimate=cost(2.0 * count * width * width + 8.0 * count * qw * span, 0),
        name="attention",
    )(*args)


def mlp(x, w_gate, w_up, w_down, layer, kind):
    count, width = x.shape
    step = min(count, 256)

    def body(x_ref, wg_ref, wu_ref, wd_ref, out_ref):
        for at in range(0, count, step):
            rows = x_ref[at : at + step]
            gate = dot_t(rows, wg_ref[...])
            upper = dot_t(rows, wu_ref[...])
            middle = (gate / (1.0 + jnp.exp(-gate)) * upper).astype(BF16)
            out_ref[at : at + step] = dot(middle, wd_ref[...]).astype(kind)

    return pl.pallas_call(
        body,
        grid=(1,),
        out_shape=jax.ShapeDtypeStruct((count, width), kind),
        in_specs=[
            whole(x.shape),
            layer_of(w_gate, layer),
            layer_of(w_up, layer),
            layer_of(w_down, layer),
        ],
        out_specs=whole((count, width)),
        compiler_params=params(28),
        cost_estimate=cost(6.0 * count * width * w_down.shape[1], 0),
        name="mlp",
    )(x, w_gate, w_up, w_down)


def last_norm(h, parts, gain):
    def body(h_ref, *refs):
        gain_ref, out_ref = refs[-2:]
        value = add_parts(h_ref[...], refs[:-2])
        out_ref[...] = norm_rows(value, gain_ref[...]).astype(BF16)

    args = [h] + parts + [gain]
    return pl.pallas_call(
        body,
        grid=(1,),
        out_shape=jax.ShapeDtypeStruct(h.shape, BF16),
        in_specs=[whole(x.shape) for x in args],
        out_specs=whole(h.shape),
        compiler_params=params(8),
        name="last_norm",
    )(*args)


def head_stats(rows, wanted, bases, shards):
    count = sum(x.shape[0] for x in rows)
    width = rows[0].shape[1]
    cols = shards[0].shape[1]
    tile = next(t for t in (1024, 768, 512, 384, 256, 128) if cols % t == 0)
    chunk = tile // 2 if tile % 256 == 0 else tile
    per = cols // tile
    steps = per * len(shards)

    def body(base_ref, want_ref, *rest):
        given = rest[: len(rows)]
        w_refs = rest[len(rows) : len(rows) + len(shards)]
        out_ref, top, total, picked, wide, x_ref = rest[len(rows) + len(shards) :]
        step = pl.program_id(0)

        @pl.when(step == 0)
        def _():
            top[...] = jnp.full_like(top, NEG)
            total[...] = jnp.zeros_like(total)
            picked[...] = jnp.zeros_like(picked)
            wide[...] = jnp.broadcast_to(want_ref[...], wide.shape)
            at = 0
            for ref in given:
                x_ref[at : at + ref.shape[0]] = ref[...]
                at += ref.shape[0]

        lane = lax.broadcasted_iota(jnp.int32, (1, LANES), 1)

        def use(w_ref, index):
            start = base_ref[index] + (step - index * per) * tile
            local = wide[...]
            for at in range(0, tile, chunk):
                logits = dot(x_ref[...], w_ref[:, at : at + chunk])
                parts = [logits[:, c : c + LANES] for c in range(0, chunk, LANES)]
                best = parts[0]
                for part in parts[1:]:
                    best = jnp.maximum(best, part)
                old = top[...]
                best = jnp.maximum(best, old)
                acc = total[...] * jnp.exp(old - best)
                pick = picked[...]
                for n, part in enumerate(parts):
                    acc = acc + jnp.exp(part - best)
                    pick = pick + jnp.where(local == lane + (start + at + n * LANES), part, 0.0)
                top[...] = best
                total[...] = acc
                picked[...] = pick

        for index, w_ref in enumerate(w_refs):
            pl.when(step // per == index)(lambda r=w_ref, n=index: use(r, n))

        @pl.when(step == steps - 1)
        def _():
            best = jnp.max(top[...], axis=1, keepdims=True)
            acc = jnp.sum(total[...] * jnp.exp(top[...] - best), axis=1, keepdims=True)
            pick = jnp.sum(picked[...], axis=1, keepdims=True)
            packed = jnp.where(lane == 0, best, jnp.where(lane == 1, acc, pick))
            out_ref[...] = jnp.transpose(packed, (1, 0))[:8]

    def column_spec(index):
        return pl.BlockSpec((width, tile), lambda s: (0, jnp.clip(s - index * per, 0, per - 1)))

    return pl.pallas_call(
        body,
        grid=(steps,),
        out_shape=jax.ShapeDtypeStruct((8, count), F32),
        in_specs=[
            pl.BlockSpec(memory_space=pltpu.SMEM),
            whole(wanted.shape),
        ]
        + [whole(x.shape) for x in rows]
        + [column_spec(n) for n in range(len(shards))],
        out_specs=whole((8, count)),
        scratch_shapes=[pltpu.VMEM((count, LANES), F32)] * 3
        + [pltpu.VMEM((count, LANES), jnp.int32), pltpu.VMEM((count, width), BF16)],
        compiler_params=params(20),
        cost_estimate=cost(2.0 * count * width * cols * len(shards), 0),
        name="head_stats",
    )(bases, wanted, *rows, *shards)


def shift(x, axes, distance, size, wrap):
    pairs = [(i, (i + distance) % size) for i in range(size) if wrap or i + distance < size]
    return lax.ppermute(x, axes, pairs)


def on_device(
    hidden_in,
    targets,
    doc_blocks,
    ref_milli,
    attn_gain,
    mlp_gain,
    final_gain,
    w_query,
    w_key,
    w_value,
    w_out,
    w_gate,
    w_up,
    w_down,
    w_head,
):
    zp_count = lax.axis_size("zp")
    core_count = lax.axis_size("core")
    dp_count = lax.axis_size(DP)
    tp_count = lax.axis_size("tensor")
    device_count = dp_count * tp_count
    row = lax.axis_index(DP)
    column = lax.axis_index("tensor")
    own_blocks, slice_len, width = hidden_in.shape
    block_len = slice_len * tp_count
    nblk = own_blocks * dp_count
    ndoc = doc_blocks.shape[0]
    tails = MAXB - 1
    own_count = own_blocks * slice_len
    vocab_shard = w_head.shape[1]

    direct = tp_count in (2, 4)

    def peer(x, k):
        return lax.ppermute(x, "tensor", [(i, i ^ k) for i in range(tp_count)])

    if core_count > 1:
        swap = [(i, core_count - 1 - i) for i in range(core_count)]
        shards = [w_head, lax.ppermute(w_head, "core", swap)]
        holders = [row, row - 2 * lax.axis_index("core") + 1]
    else:
        shards = [w_head]
        holders = [row]
    bases = jnp.stack([(r * tp_count + column) * vocab_shard for r in holders]).astype(jnp.int32)
    ids = targets.reshape(1, own_count)
    digits = jnp.concatenate([ids // 16384, ids // 128 % 128, ids % 128], axis=0).astype(BF16)
    digits = jnp.pad(digits, ((0, slice_len - 3), (0, 4 * HEAD_DIM - own_count)))[None]

    owner, offset = doc_table(doc_blocks, nblk)
    own_ids = row * own_blocks + jnp.arange(own_blocks, dtype=jnp.int32)
    slot_doc, live = lookup(own_ids, owner, nblk)
    slot_off, unused = lookup(own_ids, offset, nblk)
    prior_ids = row * own_blocks - tails + jnp.arange(tails, dtype=jnp.int32)
    prior_doc, prior_inside = lookup(prior_ids, owner, nblk)
    key_doc = jnp.concatenate([jnp.where(prior_inside, prior_doc, -1), slot_doc])
    window_doc = jnp.stack([key_doc[i : i + MAXB] for i in range(own_blocks)])
    same = (window_doc == slot_doc[:, None]) & (window_doc >= 0)
    place = column * slice_len + jnp.arange(slice_len, dtype=jnp.int32)
    inner = jnp.arange(block_len, dtype=jnp.int32)
    causal = inner[None, :] <= place[:, None]
    slot = jnp.arange(MAXB, dtype=jnp.int32)
    seen = (slot[None, :, None] < tails) | causal[:, None, :]
    bias = jnp.where(same[:, None, :, None] & seen[None], 0.0, NEG).astype(F32)
    bias = bias.reshape(own_blocks, slice_len, MAXB * block_len)

    pos = (slot_off[:, None] * block_len + place[None, :]).reshape(-1).astype(F32)
    half = HEAD_DIM // 2
    lane = jnp.arange(LANES, dtype=jnp.int32)
    freq = jnp.exp((lane % half).astype(F32) * (-2.0 * math.log(1000000.0) / HEAD_DIM))
    angle = pos[:, None] * freq[None, :]
    cosine = jnp.cos(angle)
    sine = jnp.sin(angle) * jnp.where(lane % HEAD_DIM < half, -1.0, 1.0)[None, :]

    h = hidden_in.reshape(own_count, width)
    attn_gain = tall(attn_gain)
    mlp_gain = tall(mlp_gain)
    w_gate = w_gate.transpose(0, 2, 1)
    w_up = w_up.transpose(0, 2, 1)
    parts = []
    for layer in range(w_query.shape[0]):
        h, a, kv = key_value(h, parts, attn_gain, w_key, w_value, cosine, sine, layer)
        kvw = kv.shape[1]
        kv = kv.reshape(own_blocks, slice_len, kvw)
        tail = shift(kv[own_blocks - tails :], DP, 1, dp_count, False)
        q = queries(a, w_query, cosine, sine, layer)
        kv = jnp.concatenate([tail, kv] + ([digits] if layer == 0 else []), axis=0)
        kv = lax.all_gather(kv, "tensor", axis=1, tiled=True)
        if layer == 0:
            found = kv[-1].reshape(tp_count, slice_len, kvw)[:, :3, :own_count].astype(jnp.int32)
            wanted_row = found[:, 0] * 16384 + found[:, 1] * 128 + found[:, 2]
            kv = kv[:-1]
        h, b = attention(
            q,
            kv.reshape(-1, kvw),
            bias,
            h,
            w_out,
            mlp_gain,
            layer,
        )
        if direct:
            given = [b] + [peer(b, k) for k in range(1, tp_count)]
            kinds = [F32] + [BF16] * (tp_count - 1)
            parts = [mlp(x, w_gate, w_up, w_down, layer, t) for x, t in zip(given, kinds)]
            parts = parts[:1] + [peer(parts[k], k) for k in range(1, tp_count)]
        else:
            flat = lax.all_gather(b, "tensor", axis=0, tiled=True)
            out = mlp(flat, w_gate, w_up, w_down, layer, BF16)
            out = out.reshape(tp_count, own_count, width)
            out = lax.all_to_all(out, "tensor", 0, 0, tiled=False)
            parts = [out[k] for k in range(tp_count)]
    final = last_norm(h, parts, tall(final_gain))

    zq_count = lax.axis_size("zq")
    pieces = []
    for turn_q in range(zq_count):
        for turn in range(zp_count):
            rows, wanted = final, wanted_row
            if turn:
                rows = shift(rows, "zp", turn, zp_count, True)
                wanted = shift(wanted, "zp", turn, zp_count, True)
            if turn_q:
                rows = shift(rows, "zq", turn_q, zq_count, True)
                wanted = shift(wanted, "zq", turn_q, zq_count, True)
            pieces.append((rows, wanted))
    stats = []
    first = lax.all_gather(final, "tensor", axis=0, tiled=True)
    chunk, done = [first], first
    order = [column ^ k for k in range(tp_count)]
    for n in range(len(pieces)):
        wanted = pieces[n][1]
        if n and direct:
            wanted = [lax.dynamic_slice_in_dim(wanted, k, 1, 0) for k in order]
            wanted = jnp.concatenate(wanted, axis=0)
        following = None
        if n + 1 < len(pieces):
            rows, done = lax.optimization_barrier((pieces[n + 1][0], done))
            if direct:
                following = [rows] + [peer(rows, k) for k in range(1, tp_count)]
            else:
                following = [lax.all_gather(rows, "tensor", axis=0, tiled=True)]
        stats.append(head_stats(chunk, wanted.reshape(-1, 1), bases, shards))
        chunk, done = following, stats[-1]
    stats = jnp.stack(stats)
    stats = stats.reshape(zq_count, zp_count, 8, tp_count, own_count)
    if direct:
        mixed = [jnp.take(stats, column ^ jnp.arange(tp_count), axis=3)]
        plain = stats.reshape(-1, 8, tp_count, own_count)[:1]
        mixed = mixed[0].reshape(-1, 8, tp_count, own_count)[1:]
        stats = jnp.concatenate([plain, mixed]).reshape(stats.shape)
    zp_at = (lax.axis_index("zp") - jnp.arange(zp_count)) % zp_count
    zq_at = (lax.axis_index("zq") - jnp.arange(zq_count)) % zq_count
    stats = jnp.take(jnp.take(stats, zp_at, axis=1), zq_at, axis=0)
    stats = stats[:, :, :3].transpose(1, 0, 3, 2, 4)
    stats = stats.reshape(zp_count * zq_count * tp_count, 3, own_count)
    stats = lax.all_to_all(stats, ("zp", "zq", "tensor"), 0, 0, tiled=False)
    peak = jnp.max(stats[:, 0], axis=0)
    total = jnp.sum(stats[:, 1] * jnp.exp(stats[:, 0] - peak[None]), axis=0)
    own_loss = jnp.log(total) + peak - jnp.sum(stats[:, 2], axis=0)
    own_loss = own_loss.reshape(own_blocks, slice_len)

    slot_sum = jnp.sum(own_loss, axis=1)
    hit = (slot_doc[:, None] == jnp.arange(ndoc, dtype=jnp.int32)[None, :]) & live[:, None]
    partial_docs = jnp.sum(jnp.where(hit, slot_sum[:, None], 0.0), axis=0)
    padded = jnp.pad(partial_docs, (0, LANES - ndoc))
    spread = jnp.broadcast_to(padded[None], (device_count, LANES))
    doc_total = jnp.sum(lax.all_to_all(spread, ALL, 0, 0, tiled=False), axis=0)[:ndoc]
    scores = ref_milli.astype(F32) * 0.001 - doc_total / (doc_blocks * block_len).astype(F32)
    return (own_loss, scores)


def solution(mesh):
    dp_count, tp_count = mesh.shape["dp"], mesh.shape["tensor"]
    core = 2 if dp_count % 2 == 0 else 1
    depth = dp_count // core
    pair = 2 if depth % 2 == 0 else 1
    devices = mesh.devices.reshape(depth // pair, pair, core, tp_count)
    return jax.shard_map(
        on_device,
        mesh=Mesh(devices, ALL),
        in_specs=(
            P(DP, "tensor", None),
            P(DP, "tensor"),
            P(),
            P(),
            P(),
            P(),
            P(),
            P(),
            P(),
            P(),
            P(),
            P(None, None, "tensor"),
            P(None, None, "tensor"),
            P(None, "tensor", None),
            P(None, ALL),
        ),
        out_specs=(P(DP, "tensor"), P()),
        check_vma=False,
    )
```

```python
import math

import jax
import jax.numpy as jnp
from jax import lax
from jax.experimental import pallas as pl
from jax.experimental.pallas import tpu as pltpu
from jax.sharding import Mesh
from jax.sharding import PartitionSpec as P

HEAD_DIM = 64
MAXB = 4
LANES = 128
NEG = -1e30
BF16 = jnp.bfloat16
F32 = jnp.float32
DP = ("zp", "zq", "core")
ALL = ("zp", "zq", "core", "tensor")
MIB = 1024 * 1024


def doc_table(doc_blocks, nblk):
    ends = jnp.cumsum(doc_blocks)
    starts = ends - doc_blocks
    ids = jnp.arange(nblk, dtype=jnp.int32)
    owner = jnp.sum((starts[None, :] <= ids[:, None]).astype(jnp.int32), axis=1) - 1
    hit = owner[:, None] == jnp.arange(doc_blocks.shape[0], dtype=jnp.int32)[None, :]
    first = jnp.sum(jnp.where(hit, starts[None, :], 0), axis=1)
    return (owner, ids - first)


def lookup(block_ids, table, nblk):
    hit = block_ids[:, None] == jnp.arange(nblk, dtype=jnp.int32)[None, :]
    found = jnp.sum(jnp.where(hit, table[None, :], 0), axis=1)
    inside = (block_ids >= 0) & (block_ids < nblk)
    return (found, inside)


def norm_rows(h, gain):
    scaled = h * lax.rsqrt(jnp.mean(h * h, axis=-1, keepdims=True) + 1e-06)
    return (scaled.reshape(-1, 8, h.shape[1]) * gain[None]).reshape(h.shape)


def tall(gain):
    shape = gain.shape[:-1] + (8, gain.shape[-1])
    return jnp.broadcast_to(gain[..., None, :], shape)


def dot(x, y):
    return jnp.dot(x, y, preferred_element_type=F32)


def dot_t(x, y):
    return lax.dot_general(x, y, (((1,), (1,)), ((), ())), preferred_element_type=F32)


def whole(shape):
    return pl.BlockSpec(shape, lambda *_: (0,) * len(shape))


def layer_of(array, layer):
    shape = array.shape[1:]
    return pl.BlockSpec((None,) + shape, lambda *_: (layer,) + (0,) * len(shape))


def in_hbm(x):
    return pltpu.with_memory_space_constraint(x, pltpu.HBM)


def cost(flops, moved):
    return pl.CostEstimate(flops=int(flops), bytes_accessed=int(moved), transcendentals=0)


def params(mib):
    return pltpu.CompilerParams(vmem_limit_bytes=mib * MIB)


def rotate_lanes(x, cosine, sine):
    lane = lax.broadcasted_iota(jnp.int32, (x.shape[0], LANES), 1)
    lower = lane % HEAD_DIM < HEAD_DIM // 2
    pieces = []
    for at in range(0, x.shape[1], LANES):
        part = x[:, at : at + LANES]
        other = jnp.where(
            lower,
            pltpu.roll(part, LANES - HEAD_DIM // 2, 1),
            pltpu.roll(part, HEAD_DIM // 2, 1),
        )
        pieces.append(part * cosine + other * sine)
    return pieces


def add_parts(h, refs):
    for ref in refs:
        h = h + ref[...].astype(F32)
    return h


def key_value(h, parts, gains, w_key, w_value, cosine, sine, layer):
    count, width = h.shape
    kvw = w_key.shape[-1]

    def body(*refs):
        h_ref, given, refs = refs[0], refs[1 : 1 + len(parts)], refs[1 + len(parts) :]
        value = add_parts(h_ref[...].astype(F32), given)
        gain_ref, wk_ref, wv_ref, cos_ref, sin_ref, h_out, a_out, kv_out = refs
        h_out[...] = value
        a = norm_rows(value, gain_ref[...]).astype(BF16)
        a_out[...] = a
        keys = rotate_lanes(dot(a, wk_ref[...]), cos_ref[...], sin_ref[...])
        for at, piece in enumerate(keys):
            kv_out[:, at * LANES : (at + 1) * LANES] = piece.astype(BF16)
        kv_out[:, kvw:] = dot(a, wv_ref[...]).astype(BF16)

    args = [h] + parts + [gains, in_hbm(w_key), in_hbm(w_value), cosine, sine]
    specs = [whole(x.shape) for x in args]
    specs[-5] = layer_of(gains, layer)
    specs[-4] = layer_of(w_key, layer)
    specs[-3] = layer_of(w_value, layer)
    outs = (
        jax.ShapeDtypeStruct((count, width), F32),
        jax.ShapeDtypeStruct((count, width), BF16),
        jax.ShapeDtypeStruct((count, 2 * kvw), BF16),
    )
    return pl.pallas_call(
        body,
        grid=(1,),
        out_shape=outs,
        in_specs=specs,
        out_specs=[whole(o.shape) for o in outs],
        compiler_params=params(12),
        cost_estimate=cost(2.0 * count * width * 2 * kvw, 0),
        name="key_value",
    )(*args)


def queries(a, w_query, cosine, sine, layer):
    count = a.shape[0]
    out = w_query.shape[-1]

    def body(a_ref, w_ref, cos_ref, sin_ref, q_out):
        q = rotate_lanes(dot(a_ref[...], w_ref[...]), cos_ref[...], sin_ref[...])
        for at, piece in enumerate(q):
            q_out[:, at * LANES : (at + 1) * LANES] = piece.astype(BF16)

    shape = (count, out)
    return pl.pallas_call(
        body,
        grid=(1,),
        out_shape=jax.ShapeDtypeStruct(shape, BF16),
        in_specs=[
            whole(a.shape),
            layer_of(w_query, layer),
            whole(cosine.shape),
            whole(sine.shape),
        ],
        out_specs=whole(shape),
        compiler_params=params(10),
        cost_estimate=cost(2.0 * count * out * out, 0),
        name="queries",
    )(a, in_hbm(w_query), cosine, sine)


def attention(q, tail_pieces, own_pieces, bias, h, w_out, gains, layer):
    blocks, rows, span = bias.shape
    count, qw = q.shape
    width = h.shape[1]
    kvw = own_pieces[0].shape[1] // 2
    kvh = kvw // HEAD_DIM
    heads = qw // HEAD_DIM
    group = heads // kvh
    pairs = heads // 2
    block_len = span // MAXB
    assert kvw == LANES and kvh == 2

    tails = MAXB - 1
    members = len(own_pieces)
    stride = block_len // members

    def body(*refs):
        tail_refs, own_refs, refs = refs[:members], refs[members : 2 * members], refs[2 * members :]
        q_ref, bias_ref, h_ref, gain_ref, wo_hbm, h_out, b_out = refs[:7]
        score, ctx, wo_ref, kv_ref, arrived = refs[7:]
        load = pltpu.make_async_copy(wo_hbm.at[layer], wo_ref, arrived)
        load.start()
        for member in range(members):
            for slot in range(tails + blocks):
                source = tail_refs[member] if slot < tails else own_refs[member]
                at = (slot if slot < tails else slot - tails) * stride
                to = slot * block_len + member * stride
                kv_ref[to : to + stride] = source[at : at + stride]
        low = lax.broadcasted_iota(jnp.int32, (kv_ref.shape[0], LANES), 1) < HEAD_DIM

        def variants(x, other):
            turned = pltpu.roll(x, HEAD_DIM, 1)
            return {
                (0, 0): jnp.where(low, x, other).astype(BF16),
                (1, 1): jnp.where(low, other, x).astype(BF16),
                (0, 1): jnp.where(low, turned, other).astype(BF16),
                (1, 0): jnp.where(low, other, turned).astype(BF16),
            }

        keys = variants(kv_ref[:, :kvw].astype(F32), 0.0)
        values = variants(kv_ref[:, kvw:].astype(F32), 1.0)
        work = []
        at = 0
        for i in range(blocks):
            for half in range(2):
                for c in range(kvh):
                    mine = [j for j in range(pairs) if (2 * j + half) // group == c]
                    if mine:
                        work.append((i, half, c, mine, at))
                        at += len(mine) * rows
        for i, half, c, mine, at in work:
            window = slice(i * block_len, i * block_len + span)
            stack = [q_ref[i * rows : (i + 1) * rows, j * LANES : (j + 1) * LANES] for j in mine]
            found = dot_t(jnp.concatenate(stack, axis=0), keys[(half, c)][window])
            for n in range(len(mine)):
                piece = found[n * rows : (n + 1) * rows] * HEAD_DIM ** (-0.5) + bias_ref[i]
                score[at + n * rows : at + (n + 1) * rows] = piece
        halves = {}
        for i, half, c, mine, at in work:
            window = slice(i * block_len, i * block_len + span)
            piece = score[at : at + len(mine) * rows]
            expo = jnp.exp(piece - jnp.max(piece, axis=-1, keepdims=True)).astype(BF16)
            got = dot(expo, values[(half, c)][window])
            got = got / pltpu.roll(got, HEAD_DIM, 1)
            for n, j in enumerate(mine):
                halves[(i, j, half)] = got[n * rows : (n + 1) * rows]
        first = low[:rows]
        for i in range(blocks):
            for j in range(pairs):
                ctx[i * rows : (i + 1) * rows, j * LANES : (j + 1) * LANES] = jnp.where(
                    first, halves[(i, j, 0)], halves[(i, j, 1)]
                )
        load.wait()
        value = h_ref[...] + dot(ctx[...].astype(BF16), wo_ref[...])
        h_out[...] = value
        b_out[...] = norm_rows(value, gain_ref[...]).astype(BF16)

    args = [*tail_pieces, *own_pieces, q, bias, h, gains, in_hbm(w_out)]
    specs = [whole(x.shape) for x in args]
    specs[-2] = layer_of(gains, layer)
    specs[-1] = pl.BlockSpec(memory_space=pl.ANY)
    outs = (
        jax.ShapeDtypeStruct((count, width), F32),
        jax.ShapeDtypeStruct((count, width), BF16),
    )
    return pl.pallas_call(
        body,
        grid=(1,),
        out_shape=outs,
        in_specs=specs,
        out_specs=[whole(o.shape) for o in outs],
        scratch_shapes=[
            pltpu.VMEM((blocks * heads * rows, span), F32),
            pltpu.VMEM((count, qw), F32),
            pltpu.VMEM((qw, width), BF16),
            pltpu.VMEM(((tails + blocks) * block_len, 2 * kvw), BF16),
            pltpu.SemaphoreType.DMA,
        ],
        compiler_params=params(20),
        cost_estimate=cost(2.0 * count * width * width + 8.0 * count * qw * span, 0),
        name="attention",
    )(*args)


def mlp(x, w_gate, w_up, w_down, layer, kind):
    count, width = x.shape
    step = min(count, 256)

    def body(x_ref, wg_ref, wu_ref, wd_ref, out_ref):
        for at in range(0, count, step):
            rows = x_ref[at : at + step]
            gate = dot_t(rows, wg_ref[...])
            upper = dot_t(rows, wu_ref[...])
            middle = (gate / (1.0 + jnp.exp(-gate)) * upper).astype(BF16)
            out_ref[at : at + step] = dot(middle, wd_ref[...]).astype(kind)

    return pl.pallas_call(
        body,
        grid=(1,),
        out_shape=jax.ShapeDtypeStruct((count, width), kind),
        in_specs=[
            whole(x.shape),
            layer_of(w_gate, layer),
            layer_of(w_up, layer),
            layer_of(w_down, layer),
        ],
        out_specs=whole((count, width)),
        compiler_params=params(28),
        cost_estimate=cost(6.0 * count * width * w_down.shape[1], 0),
        name="mlp",
    )(x, w_gate, w_up, w_down)


def mlp_rows(rows, wg, wu, wd):
    gate = dot_t(rows, wg[...])
    upper = dot_t(rows, wu[...])
    return dot((gate / (1.0 + jnp.exp(-gate)) * upper).astype(BF16), wd[...])


def mlp_load(x, w_gate, w_up, w_down, layer):
    stacks = (w_gate, w_up, w_down)

    def body(x_ref, *refs):
        sources, out_ref, kept, arrived = refs[:3], refs[3], refs[4:7], refs[7]
        loads = [
            pltpu.make_async_copy(source.at[layer], target, arrived.at[n])
            for n, (source, target) in enumerate(zip(sources, kept))
        ]
        for load in loads:
            load.start()
        for load in loads:
            load.wait()
        out_ref[...] = mlp_rows(x_ref[...], *kept)

    return pl.pallas_call(
        body,
        grid=(1,),
        out_shape=[jax.ShapeDtypeStruct(x.shape, F32)]
        + [pltpu.VMEM(w.shape[1:], BF16) for w in stacks],
        in_specs=[whole(x.shape)] + [pl.BlockSpec(memory_space=pl.ANY)] * 3,
        out_specs=[whole(x.shape)] + [pl.BlockSpec(memory_space=pltpu.VMEM)] * 3,
        scratch_shapes=[pltpu.SemaphoreType.DMA((3,))],
        compiler_params=params(12),
        cost_estimate=cost(6.0 * x.size * w_down.shape[1], 0),
        name="mlp_load",
    )(x, *[in_hbm(w) for w in stacks])


def mlp_kept(x, weights):
    def body(x_ref, wg_ref, wu_ref, wd_ref, out_ref):
        out_ref[...] = mlp_rows(x_ref[...], wg_ref, wu_ref, wd_ref).astype(BF16)

    return pl.pallas_call(
        body,
        grid=(1,),
        out_shape=jax.ShapeDtypeStruct(x.shape, BF16),
        in_specs=[whole(x.shape)] + [pl.BlockSpec(memory_space=pltpu.VMEM)] * 3,
        out_specs=whole(x.shape),
        compiler_params=params(12),
        cost_estimate=cost(6.0 * x.size * weights[2].shape[0], 0),
        name="mlp_kept",
    )(x, *[pltpu.with_memory_space_constraint(w, pltpu.VMEM) for w in weights])


def last_norm(h, parts, gain):
    def body(h_ref, *refs):
        gain_ref, out_ref = refs[-2:]
        value = add_parts(h_ref[...], refs[:-2])
        out_ref[...] = norm_rows(value, gain_ref[...]).astype(BF16)

    args = [h] + parts + [gain]
    return pl.pallas_call(
        body,
        grid=(1,),
        out_shape=jax.ShapeDtypeStruct(h.shape, BF16),
        in_specs=[whole(x.shape) for x in args],
        out_specs=whole(h.shape),
        compiler_params=params(8),
        name="last_norm",
    )(*args)


def head_stats(rows, wanted, bases, shards):
    count = sum(x.shape[0] for x in rows)
    width = rows[0].shape[1]
    cols = shards[0].shape[1]
    tile = next(t for t in (1024, 768, 512, 384, 256, 128) if cols % t == 0)
    chunk = tile // 2 if tile % 256 == 0 else tile
    per = cols // tile
    steps = per * len(shards)

    def body(base_ref, want_ref, *rest):
        given = rest[: len(rows)]
        w_refs = rest[len(rows) : len(rows) + len(shards)]
        out_ref, top, total, picked, wide, x_ref = rest[len(rows) + len(shards) :]
        step = pl.program_id(0)

        @pl.when(step == 0)
        def _():
            top[...] = jnp.full_like(top, NEG)
            total[...] = jnp.zeros_like(total)
            picked[...] = jnp.zeros_like(picked)
            wide[...] = jnp.broadcast_to(want_ref[...], wide.shape)
            at = 0
            for ref in given:
                x_ref[at : at + ref.shape[0]] = ref[...]
                at += ref.shape[0]

        lane = lax.broadcasted_iota(jnp.int32, (1, LANES), 1)

        def use(w_ref, index):
            start = base_ref[index] + (step - index * per) * tile
            local = wide[...]
            for at in range(0, tile, chunk):
                logits = dot(x_ref[...], w_ref[:, at : at + chunk])
                parts = [logits[:, c : c + LANES] for c in range(0, chunk, LANES)]
                best = parts[0]
                for part in parts[1:]:
                    best = jnp.maximum(best, part)
                old = top[...]
                best = jnp.maximum(best, old)
                acc = total[...] * jnp.exp(old - best)
                pick = picked[...]
                for n, part in enumerate(parts):
                    acc = acc + jnp.exp(part - best)
                    pick = pick + jnp.where(local == lane + (start + at + n * LANES), part, 0.0)
                top[...] = best
                total[...] = acc
                picked[...] = pick

        for index, w_ref in enumerate(w_refs):
            pl.when(step // per == index)(lambda r=w_ref, n=index: use(r, n))

        @pl.when(step == steps - 1)
        def _():
            best = jnp.max(top[...], axis=1, keepdims=True)
            acc = jnp.sum(total[...] * jnp.exp(top[...] - best), axis=1, keepdims=True)
            pick = jnp.sum(picked[...], axis=1, keepdims=True)
            packed = jnp.where(lane == 0, best, jnp.where(lane == 1, acc, pick))
            out_ref[...] = jnp.transpose(packed, (1, 0))[:8]

    def column_spec(index):
        return pl.BlockSpec((width, tile), lambda s: (0, jnp.clip(s - index * per, 0, per - 1)))

    return pl.pallas_call(
        body,
        grid=(steps,),
        out_shape=jax.ShapeDtypeStruct((8, count), F32),
        in_specs=[
            pl.BlockSpec(memory_space=pltpu.SMEM),
            whole(wanted.shape),
        ]
        + [whole(x.shape) for x in rows]
        + [column_spec(n) for n in range(len(shards))],
        out_specs=whole((8, count)),
        scratch_shapes=[pltpu.VMEM((count, LANES), F32)] * 3
        + [pltpu.VMEM((count, LANES), jnp.int32), pltpu.VMEM((count, width), BF16)],
        compiler_params=params(20),
        cost_estimate=cost(2.0 * count * width * cols * len(shards), 0),
        name="head_stats",
    )(bases, wanted, *rows, *[in_hbm(w) for w in shards])


def head_stats_mxu(rows, wanted, bases, shards):
    count = sum(x.shape[0] for x in rows)
    width = rows[0].shape[1]
    cols = shards[0].shape[1]
    deep, pair = 256, 512
    tile = 2 * pair
    per = cols // tile
    steps = per * len(shards)
    full, rest_k = width // deep, width % deep
    starts = [k * deep for k in range(full)] + ([width - deep] if rest_k else [])
    pieces = len(starts)
    piece = count // pieces
    padded = len(starts) * deep
    cuts = 7 if width % 112 == 0 else 1

    def body(base_ref, want_ref, *refs):
        given = refs[: len(rows)]
        sources = refs[len(rows) : len(rows) + len(shards)]
        out_ref, top, total, picked, wide, x_ref, w_buf, arrived = refs[len(rows) + len(shards) :]
        lane = lax.broadcasted_iota(jnp.int32, (1, LANES), 1)

        def copy_part(source, at, slot, n):
            part = pl.ds(n * (width // cuts), width // cuts)
            return pltpu.make_async_copy(
                source.at[part, pl.ds(at, tile)], w_buf.at[slot, part], arrived.at[slot, n]
            )

        def fetch(step):
            for index, source in enumerate(sources):

                @pl.when(step // per == index)
                def _(source=source, index=index):
                    at = pl.multiple_of((step - index * per) * tile, tile)
                    for n in range(cuts):
                        copy_part(source, at, step % 2, n).start()

        def column(step):
            start = base_ref[0] + step * tile
            for index in range(1, len(shards)):
                here = base_ref[index] + (step - index * per) * tile
                start = jnp.where(step >= index * per, here, start)
            return start

        def scoped(*accs):
            fetch(0)
            top[...] = jnp.full_like(top, NEG)
            total[...] = jnp.zeros_like(total)
            picked[...] = jnp.zeros_like(picked)
            wide[...] = jnp.broadcast_to(want_ref[...], wide.shape)
            at = 0
            for ref in given:
                size = ref.shape[0]
                x_ref[at : at + size, : full * deep] = ref[:, : full * deep]
                if rest_k:
                    blank = jnp.zeros((size, deep - rest_k), BF16)
                    x_ref[at : at + size, full * deep : padded - rest_k] = blank
                    x_ref[at : at + size, padded - rest_k :] = ref[:, full * deep :]
                at += size
            half = [[accs[(b * 2 + q) * pieces :][:pieces] for q in range(2)] for b in range(2)]

            def multiply(b, slot, k):
                for q in range(2):
                    at = b * pair + q * deep
                    register = k % 2
                    pltpu.matmul_push_rhs(
                        w_buf[slot, starts[k] : starts[k] + deep, at : at + deep],
                        staging_register=register,
                        mxu_index=q,
                    )
                    for n in range(pieces):
                        pltpu.matmul_acc_lhs(
                            half[b][q][n],
                            x_ref[n * piece : (n + 1) * piece, k * deep : (k + 1) * deep],
                            load_staged_rhs=register if n == 0 else None,
                        )

            def collect(b, n, start, fresh):
                at = slice(n * piece, (n + 1) * piece)
                parts = []
                for q in range(2):
                    found = pltpu.matmul_pop(half[b][q][n])
                    parts += [found[:, c : c + LANES] for c in range(0, deep, LANES)]
                best = parts[0]
                for part in parts[1:]:
                    best = jnp.maximum(best, part)
                old = top[at]
                best = jnp.maximum(best, old)
                acc = total[at] * jnp.exp(old - best)
                pick = picked[at]
                local = wide[at]
                for c, part in enumerate(parts):
                    acc = acc + jnp.exp(part - best)
                    pick = pick + jnp.where(local == lane + (start + c * LANES), part, 0.0)
                if fresh is not None:
                    best = jnp.where(fresh, NEG, best)
                    acc = jnp.where(fresh, 0.0, acc)
                    pick = jnp.where(fresh, 0.0, pick)
                top[at] = best
                total[at] = acc
                picked[at] = pick

            def step_fn(step, carry):
                slot = step % 2
                for n in range(cuts):
                    copy_part(sources[0], 0, slot, n).wait()
                pl.when(step + 1 < steps)(lambda: fetch(step + 1))
                before = column(jnp.maximum(step - 1, 0)) + pair
                start = column(step)
                for k in range(len(starts)):
                    multiply(0, slot, k)
                    collect(1, k, before, step == 0)
                for k in range(len(starts)):
                    multiply(1, slot, k)
                    collect(0, k, start, None)
                return carry

            lax.fori_loop(0, steps, step_fn, 0)
            for k in range(pieces):
                collect(1, k, column(steps - 1) + pair, None)
            best = jnp.max(top[...], axis=1, keepdims=True)
            acc = jnp.sum(total[...] * jnp.exp(top[...] - best), axis=1, keepdims=True)
            pick = jnp.sum(picked[...], axis=1, keepdims=True)
            packed = jnp.where(lane == 0, best, jnp.where(lane == 1, acc, pick))
            out_ref[...] = jnp.transpose(packed, (1, 0))[:8]

        kinds = [pltpu.ACC(q)((piece, deep), F32) for b in range(2) for q in range(2) for n in range(pieces)]
        pl.run_scoped(scoped, *kinds)

    return pl.pallas_call(
        body,
        grid=(1,),
        out_shape=jax.ShapeDtypeStruct((8, count), F32),
        in_specs=[
            pl.BlockSpec(memory_space=pltpu.SMEM),
            whole(wanted.shape),
        ]
        + [whole(x.shape) for x in rows]
        + [pl.BlockSpec(memory_space=pl.ANY)] * len(shards),
        out_specs=whole((8, count)),
        scratch_shapes=[pltpu.VMEM((count, LANES), F32)] * 3
        + [
            pltpu.VMEM((count, LANES), jnp.int32),
            pltpu.VMEM((count, padded), BF16),
            pltpu.VMEM((2, width, tile), BF16),
            pltpu.SemaphoreType.DMA((2, cuts)),
        ],
        compiler_params=params(20),
        cost_estimate=cost(2.0 * count * width * cols * len(shards), 0),
        name="head_stats_mxu",
    )(bases, wanted, *rows, *[in_hbm(w) for w in shards])


def shift(x, axes, distance, size, wrap):
    pairs = [(i, (i + distance) % size) for i in range(size) if wrap or i + distance < size]
    return lax.ppermute(x, axes, pairs)


def on_device(
    hidden_in,
    targets,
    doc_blocks,
    ref_milli,
    attn_gain,
    mlp_gain,
    final_gain,
    w_query,
    w_key,
    w_value,
    w_out,
    w_gate,
    w_up,
    w_down,
    w_head,
):
    zp_count = lax.axis_size("zp")
    core_count = lax.axis_size("core")
    dp_count = lax.axis_size(DP)
    tp_count = lax.axis_size("tensor")
    device_count = dp_count * tp_count
    row = lax.axis_index(DP)
    column = lax.axis_index("tensor")
    own_blocks, slice_len, width = hidden_in.shape
    block_len = slice_len * tp_count
    nblk = own_blocks * dp_count
    ndoc = doc_blocks.shape[0]
    tails = MAXB - 1
    own_count = own_blocks * slice_len
    vocab_shard = w_head.shape[1]

    direct = tp_count in (2, 4)

    def peer(x, k):
        return lax.ppermute(x, "tensor", [(i, i ^ k) for i in range(tp_count)])

    if core_count > 1:
        swap = [(i, core_count - 1 - i) for i in range(core_count)]
        shards = [w_head, lax.ppermute(w_head, "core", swap)]
        holders = [row, row - 2 * lax.axis_index("core") + 1]
    else:
        shards = [w_head]
        holders = [row]
    bases = jnp.stack([(r * tp_count + column) * vocab_shard for r in holders]).astype(jnp.int32)
    ids = targets.reshape(1, own_count)
    digits = jnp.concatenate([ids // 16384, ids // 128 % 128, ids % 128], axis=0).astype(BF16)
    digits = jnp.pad(digits, ((0, slice_len - 3), (0, 2 * w_key.shape[-1] - own_count)))

    owner, offset = doc_table(doc_blocks, nblk)
    own_ids = row * own_blocks + jnp.arange(own_blocks, dtype=jnp.int32)
    slot_doc, live = lookup(own_ids, owner, nblk)
    slot_off, unused = lookup(own_ids, offset, nblk)
    prior_ids = row * own_blocks - tails + jnp.arange(tails, dtype=jnp.int32)
    prior_doc, prior_inside = lookup(prior_ids, owner, nblk)
    key_doc = jnp.concatenate([jnp.where(prior_inside, prior_doc, -1), slot_doc])
    window_doc = jnp.stack([key_doc[i : i + MAXB] for i in range(own_blocks)])
    same = (window_doc == slot_doc[:, None]) & (window_doc >= 0)
    place = column * slice_len + jnp.arange(slice_len, dtype=jnp.int32)
    inner = jnp.arange(block_len, dtype=jnp.int32)
    causal = inner[None, :] <= place[:, None]
    slot = jnp.arange(MAXB, dtype=jnp.int32)
    seen = (slot[None, :, None] < tails) | causal[:, None, :]
    bias = jnp.where(same[:, None, :, None] & seen[None], 0.0, NEG).astype(F32)
    bias = bias.reshape(own_blocks, slice_len, MAXB * block_len)

    pos = (slot_off[:, None] * block_len + place[None, :]).reshape(-1).astype(F32)
    half = HEAD_DIM // 2
    lane = jnp.arange(LANES, dtype=jnp.int32)
    freq = jnp.exp((lane % half).astype(F32) * (-2.0 * math.log(1000000.0) / HEAD_DIM))
    angle = pos[:, None] * freq[None, :]
    cosine = jnp.cos(angle)
    sine = jnp.sin(angle) * jnp.where(lane % HEAD_DIM < half, -1.0, 1.0)[None, :]

    h = hidden_in.reshape(own_count, width)
    attn_gain = tall(attn_gain)
    mlp_gain = tall(mlp_gain)
    w_gate = w_gate.transpose(0, 2, 1)
    w_up = w_up.transpose(0, 2, 1)
    parts = []
    for layer in range(w_query.shape[0]):
        h, a, kv = key_value(h, parts, attn_gain, w_key, w_value, cosine, sine, layer)
        kvw = kv.shape[1]
        kv = kv.reshape(own_blocks, slice_len, kvw)
        tail = shift(kv[own_blocks - tails :], DP, 1, dp_count, False)
        q = queries(a, w_query, cosine, sine, layer)
        kv = jnp.concatenate([tail, kv] + ([digits[None]] if layer == 0 else []), axis=0)
        kv = lax.all_gather(kv, "tensor", axis=1, tiled=True)
        if layer == 0:
            found = kv[-1].reshape(tp_count, slice_len, kvw)[:, :3, :own_count].astype(jnp.int32)
            wanted_row = found[:, 0] * 16384 + found[:, 1] * 128 + found[:, 2]
            kv = kv[:-1]
        tail_pieces = [kv[:tails].reshape(-1, kvw)]
        own_pieces = [kv[tails:].reshape(-1, kvw)]
        h, b = attention(
            q,
            tail_pieces,
            own_pieces,
            bias,
            h,
            w_out,
            mlp_gain,
            layer,
        )
        if direct:
            given = [peer(b, k) for k in range(1, tp_count)]
            mine, *kept = mlp_load(b, w_gate, w_up, w_down, layer)
            parts = [mine]
            for k, x in enumerate(given, 1):
                parts.append(peer(mlp_kept(x, kept), k))
        else:
            flat = lax.all_gather(b, "tensor", axis=0, tiled=True)
            out = mlp(flat, w_gate, w_up, w_down, layer, BF16)
            out = out.reshape(tp_count, own_count, width)
            out = lax.all_to_all(out, "tensor", 0, 0, tiled=False)
            parts = [out[k] for k in range(tp_count)]
    final = last_norm(h, parts, tall(final_gain))

    zq_count = lax.axis_size("zq")
    turns = [(q, p) for q in range(zq_count) for p in range(zp_count)]

    def brought(x, turn):
        if turn == (0, 0):
            return x
        route = [
            (p * zq_count + q, (p + turn[1]) % zp_count * zq_count + (q + turn[0]) % zq_count)
            for p in range(zp_count)
            for q in range(zq_count)
        ]
        return lax.ppermute(x, ("zp", "zq"), route)

    def gathered(x):
        if direct:
            return [x] + [peer(x, k) for k in range(1, tp_count)]
        return [lax.all_gather(x, "tensor", axis=0, tiled=True)]

    if direct:
        order = [column ^ k for k in range(tp_count)]
        wanted_row = [lax.dynamic_slice_in_dim(wanted_row, k, 1, 0) for k in order]
        wanted_row = jnp.concatenate(wanted_row)
    wanted = [brought(wanted_row, turn).reshape(-1, 1) for turn in turns]
    chunk = gathered(final)
    done = chunk[-1]
    queue = [brought(final, turn) for turn in turns[1:3]]
    stats = []
    for n in range(len(turns)):
        following = None
        if n + 1 < len(turns):
            ahead, source, done = lax.optimization_barrier((queue.pop(0), final, done))
            following = gathered(ahead)
            if n + 3 < len(turns):
                queue.append(brought(source, turns[n + 3]))
        fits = vocab_shard % 1024 == 0 and sum(x.shape[0] for x in chunk) % 64 == 0
        stage = head_stats_mxu if fits else head_stats
        stats.append(stage(chunk, wanted[n], bases, shards))
        chunk = following
        bases, done = lax.optimization_barrier((bases, stats[-1]))
        stats[-1] = done
    stats = jnp.stack(stats)[:, :3].reshape(len(turns), 3, tp_count, own_count)
    stats = stats.transpose(0, 2, 1, 3).reshape(-1, 3, own_count)
    place_zp = jnp.arange(zp_count)[:, None, None]
    place_zq = jnp.arange(zq_count)[None, :, None]
    place_t = jnp.arange(tp_count)[None, None, :]
    at = (lax.axis_index("zq") - place_zq) % zq_count * zp_count
    at = (at + (lax.axis_index("zp") - place_zp) % zp_count) * tp_count
    at = at + (place_t ^ column if direct else place_t)
    stats = jnp.take(stats, at.reshape(-1), axis=0, mode="clip")
    stats = lax.all_to_all(stats, ("zp", "zq", "tensor"), 0, 0, tiled=False)
    peak = jnp.max(stats[:, 0], axis=0)
    total = jnp.sum(stats[:, 1] * jnp.exp(stats[:, 0] - peak[None]), axis=0)
    own_loss = jnp.log(total) + peak - jnp.sum(stats[:, 2], axis=0)
    own_loss = own_loss.reshape(own_blocks, slice_len)

    slot_sum = jnp.sum(own_loss, axis=1)
    hit = (slot_doc[:, None] == jnp.arange(ndoc, dtype=jnp.int32)[None, :]) & live[:, None]
    partial_docs = jnp.sum(jnp.where(hit, slot_sum[:, None], 0.0), axis=0)
    padded = jnp.pad(partial_docs, (0, LANES - ndoc))
    spread = jnp.broadcast_to(padded[None], (device_count, LANES))
    doc_total = jnp.sum(lax.all_to_all(spread, ALL, 0, 0, tiled=False), axis=0)[:ndoc]
    scores = ref_milli.astype(F32) * 0.001 - doc_total / (doc_blocks * block_len).astype(F32)
    return (own_loss, scores)


def solution(mesh):
    dp_count, tp_count = mesh.shape["dp"], mesh.shape["tensor"]
    core = 2 if dp_count % 2 == 0 else 1
    depth = dp_count // core
    pair = 2 if depth % 2 == 0 else 1
    devices = mesh.devices.reshape(depth // pair, pair, core, tp_count)
    return jax.shard_map(
        on_device,
        mesh=Mesh(devices, ALL),
        in_specs=(
            P(DP, "tensor", None),
            P(DP, "tensor"),
            P(),
            P(),
            P(),
            P(),
            P(),
            P(),
            P(),
            P(),
            P(),
            P(None, None, "tensor"),
            P(None, None, "tensor"),
            P(None, "tensor", None),
            P(None, ALL),
        ),
        out_specs=(P(DP, "tensor"), P()),
        check_vma=False,
    )
```

```python
import math

import jax
import jax.numpy as jnp
from jax import lax
from jax.experimental import pallas as pl
from jax.experimental.pallas import tpu as pltpu
from jax.sharding import Mesh
from jax.sharding import PartitionSpec as P

HEAD_DIM = 64
MAXB = 4
LANES = 128
NEG = -1e30
BF16 = jnp.bfloat16
F32 = jnp.float32
DP = ("zp", "zq", "core")
ALL = ("zp", "zq", "core", "tensor")
MIB = 1024 * 1024


def doc_table(doc_blocks, nblk):
    ends = jnp.cumsum(doc_blocks)
    starts = ends - doc_blocks
    ids = jnp.arange(nblk, dtype=jnp.int32)
    owner = jnp.sum((starts[None, :] <= ids[:, None]).astype(jnp.int32), axis=1) - 1
    hit = owner[:, None] == jnp.arange(doc_blocks.shape[0], dtype=jnp.int32)[None, :]
    first = jnp.sum(jnp.where(hit, starts[None, :], 0), axis=1)
    return (owner, ids - first)


def lookup(block_ids, table, nblk):
    hit = block_ids[:, None] == jnp.arange(nblk, dtype=jnp.int32)[None, :]
    found = jnp.sum(jnp.where(hit, table[None, :], 0), axis=1)
    inside = (block_ids >= 0) & (block_ids < nblk)
    return (found, inside)


def norm_rows(h, gain):
    scaled = h * lax.rsqrt(jnp.mean(h * h, axis=-1, keepdims=True) + 1e-06)
    return (scaled.reshape(-1, 8, h.shape[1]) * gain[None]).reshape(h.shape)


def tall(gain):
    shape = gain.shape[:-1] + (8, gain.shape[-1])
    return jnp.broadcast_to(gain[..., None, :], shape)


def dot(x, y):
    return jnp.dot(x, y, preferred_element_type=F32)


def dot_t(x, y):
    return lax.dot_general(x, y, (((1,), (1,)), ((), ())), preferred_element_type=F32)


def whole(shape):
    return pl.BlockSpec(shape, lambda *_: (0,) * len(shape))


def layer_of(array, layer):
    shape = array.shape[1:]
    return pl.BlockSpec((None,) + shape, lambda *_: (layer,) + (0,) * len(shape))


def in_hbm(x):
    return pltpu.with_memory_space_constraint(x, pltpu.HBM)


def cost(flops, moved):
    return pl.CostEstimate(flops=int(flops), bytes_accessed=int(moved), transcendentals=0)


def params(mib):
    return pltpu.CompilerParams(vmem_limit_bytes=mib * MIB)


def rotate_lanes(x, cosine, sine):
    lane = lax.broadcasted_iota(jnp.int32, (x.shape[0], LANES), 1)
    lower = lane % HEAD_DIM < HEAD_DIM // 2
    pieces = []
    for at in range(0, x.shape[1], LANES):
        part = x[:, at : at + LANES]
        other = jnp.where(
            lower,
            pltpu.roll(part, LANES - HEAD_DIM // 2, 1),
            pltpu.roll(part, HEAD_DIM // 2, 1),
        )
        pieces.append(part * cosine + other * sine)
    return pieces


def add_parts(h, refs):
    for ref in refs:
        h = h + ref[...].astype(F32)
    return h


def key_value(h, parts, gains, w_key, w_value, cosine, sine, layer):
    count, width = h.shape
    kvw = w_key.shape[-1]

    def body(*refs):
        h_ref, given, refs = refs[0], refs[1 : 1 + len(parts)], refs[1 + len(parts) :]
        value = add_parts(h_ref[...].astype(F32), given)
        gain_ref, wk_ref, wv_ref, cos_ref, sin_ref, h_out, a_out, kv_out = refs
        h_out[...] = value
        a = norm_rows(value, gain_ref[...]).astype(BF16)
        a_out[...] = a
        keys = rotate_lanes(dot(a, wk_ref[...]), cos_ref[...], sin_ref[...])
        for at, piece in enumerate(keys):
            kv_out[:, at * LANES : (at + 1) * LANES] = piece.astype(BF16)
        kv_out[:, kvw:] = dot(a, wv_ref[...]).astype(BF16)

    args = [h] + parts + [gains, in_hbm(w_key), in_hbm(w_value), cosine, sine]
    specs = [whole(x.shape) for x in args]
    specs[-5] = layer_of(gains, layer)
    specs[-4] = layer_of(w_key, layer)
    specs[-3] = layer_of(w_value, layer)
    outs = (
        jax.ShapeDtypeStruct((count, width), F32),
        jax.ShapeDtypeStruct((count, width), BF16),
        jax.ShapeDtypeStruct((count, 2 * kvw), BF16),
    )
    return pl.pallas_call(
        body,
        grid=(1,),
        out_shape=outs,
        in_specs=specs,
        out_specs=[whole(o.shape) for o in outs],
        compiler_params=params(12),
        cost_estimate=cost(2.0 * count * width * 2 * kvw, 0),
        name="key_value",
    )(*args)


def queries(a, w_query, cosine, sine, layer):
    count = a.shape[0]
    out = w_query.shape[-1]

    def body(a_ref, w_ref, cos_ref, sin_ref, q_out):
        q = rotate_lanes(dot(a_ref[...], w_ref[...]), cos_ref[...], sin_ref[...])
        for at, piece in enumerate(q):
            q_out[:, at * LANES : (at + 1) * LANES] = piece.astype(BF16)

    shape = (count, out)
    return pl.pallas_call(
        body,
        grid=(1,),
        out_shape=jax.ShapeDtypeStruct(shape, BF16),
        in_specs=[
            whole(a.shape),
            layer_of(w_query, layer),
            whole(cosine.shape),
            whole(sine.shape),
        ],
        out_specs=whole(shape),
        compiler_params=params(10),
        cost_estimate=cost(2.0 * count * out * out, 0),
        name="queries",
    )(a, in_hbm(w_query), cosine, sine)


def attention(q, tail_pieces, own_pieces, bias, h, w_out, gains, layer):
    blocks, rows, span = bias.shape
    count, qw = q.shape
    width = h.shape[1]
    kvw = own_pieces[0].shape[1] // 2
    kvh = kvw // HEAD_DIM
    heads = qw // HEAD_DIM
    group = heads // kvh
    pairs = heads // 2
    block_len = span // MAXB
    assert kvw == LANES and kvh == 2

    tails = MAXB - 1
    members = len(own_pieces)
    stride = block_len // members

    def body(*refs):
        tail_refs, own_refs, refs = refs[:members], refs[members : 2 * members], refs[2 * members :]
        q_ref, bias_ref, h_ref, gain_ref, wo_hbm, h_out, b_out = refs[:7]
        score, ctx, wo_ref, kv_ref, arrived = refs[7:]
        load = pltpu.make_async_copy(wo_hbm.at[layer], wo_ref, arrived)
        load.start()
        for member in range(members):
            for slot in range(tails + blocks):
                source = tail_refs[member] if slot < tails else own_refs[member]
                at = (slot if slot < tails else slot - tails) * stride
                to = slot * block_len + member * stride
                kv_ref[to : to + stride] = source[at : at + stride]
        low = lax.broadcasted_iota(jnp.int32, (kv_ref.shape[0], LANES), 1) < HEAD_DIM

        def variants(x, other):
            turned = pltpu.roll(x, HEAD_DIM, 1)
            return {
                (0, 0): jnp.where(low, x, other).astype(BF16),
                (1, 1): jnp.where(low, other, x).astype(BF16),
                (0, 1): jnp.where(low, turned, other).astype(BF16),
                (1, 0): jnp.where(low, other, turned).astype(BF16),
            }

        keys = variants(kv_ref[:, :kvw].astype(F32), 0.0)
        values = variants(kv_ref[:, kvw:].astype(F32), 1.0)
        work = []
        at = 0
        for i in range(blocks):
            for half in range(2):
                for c in range(kvh):
                    mine = [j for j in range(pairs) if (2 * j + half) // group == c]
                    if mine:
                        work.append((i, half, c, mine, at))
                        at += len(mine) * rows
        for i, half, c, mine, at in work:
            window = slice(i * block_len, i * block_len + span)
            stack = [q_ref[i * rows : (i + 1) * rows, j * LANES : (j + 1) * LANES] for j in mine]
            found = dot_t(jnp.concatenate(stack, axis=0), keys[(half, c)][window])
            for n in range(len(mine)):
                piece = found[n * rows : (n + 1) * rows] * HEAD_DIM ** (-0.5) + bias_ref[i]
                score[at + n * rows : at + (n + 1) * rows] = piece
        halves = {}
        for i, half, c, mine, at in work:
            window = slice(i * block_len, i * block_len + span)
            piece = score[at : at + len(mine) * rows]
            expo = jnp.exp(piece - jnp.max(piece, axis=-1, keepdims=True)).astype(BF16)
            got = dot(expo, values[(half, c)][window])
            got = got / pltpu.roll(got, HEAD_DIM, 1)
            for n, j in enumerate(mine):
                halves[(i, j, half)] = got[n * rows : (n + 1) * rows]
        first = low[:rows]
        for i in range(blocks):
            for j in range(pairs):
                ctx[i * rows : (i + 1) * rows, j * LANES : (j + 1) * LANES] = jnp.where(
                    first, halves[(i, j, 0)], halves[(i, j, 1)]
                )
        load.wait()
        value = h_ref[...] + dot(ctx[...].astype(BF16), wo_ref[...])
        h_out[...] = value
        b_out[...] = norm_rows(value, gain_ref[...]).astype(BF16)

    args = [*tail_pieces, *own_pieces, q, bias, h, gains, in_hbm(w_out)]
    specs = [whole(x.shape) for x in args]
    specs[-2] = layer_of(gains, layer)
    specs[-1] = pl.BlockSpec(memory_space=pl.ANY)
    outs = (
        jax.ShapeDtypeStruct((count, width), F32),
        jax.ShapeDtypeStruct((count, width), BF16),
    )
    return pl.pallas_call(
        body,
        grid=(1,),
        out_shape=outs,
        in_specs=specs,
        out_specs=[whole(o.shape) for o in outs],
        scratch_shapes=[
            pltpu.VMEM((blocks * heads * rows, span), F32),
            pltpu.VMEM((count, qw), F32),
            pltpu.VMEM((qw, width), BF16),
            pltpu.VMEM(((tails + blocks) * block_len, 2 * kvw), BF16),
            pltpu.SemaphoreType.DMA,
        ],
        compiler_params=params(20),
        cost_estimate=cost(2.0 * count * width * width + 8.0 * count * qw * span, 0),
        name="attention",
    )(*args)


def mlp(x, w_gate, w_up, w_down, layer, kind):
    count, width = x.shape
    step = min(count, 256)

    def body(x_ref, wg_ref, wu_ref, wd_ref, out_ref):
        for at in range(0, count, step):
            rows = x_ref[at : at + step]
            gate = dot_t(rows, wg_ref[...])
            upper = dot_t(rows, wu_ref[...])
            middle = (gate / (1.0 + jnp.exp(-gate)) * upper).astype(BF16)
            out_ref[at : at + step] = dot(middle, wd_ref[...]).astype(kind)

    return pl.pallas_call(
        body,
        grid=(1,),
        out_shape=jax.ShapeDtypeStruct((count, width), kind),
        in_specs=[
            whole(x.shape),
            layer_of(w_gate, layer),
            layer_of(w_up, layer),
            layer_of(w_down, layer),
        ],
        out_specs=whole((count, width)),
        compiler_params=params(28),
        cost_estimate=cost(6.0 * count * width * w_down.shape[1], 0),
        name="mlp",
    )(x, w_gate, w_up, w_down)


def mlp_rows(rows, wg, wu, wd):
    gate = dot_t(rows, wg[...])
    upper = dot_t(rows, wu[...])
    return dot((gate / (1.0 + jnp.exp(-gate)) * upper).astype(BF16), wd[...])


def mlp_load(x, w_gate, w_up, w_down, layer):
    stacks = (w_gate, w_up, w_down)

    def body(x_ref, *refs):
        sources, out_ref, kept, arrived = refs[:3], refs[3], refs[4:7], refs[7]
        loads = [
            pltpu.make_async_copy(source.at[layer], target, arrived.at[n])
            for n, (source, target) in enumerate(zip(sources, kept))
        ]
        for load in loads:
            load.start()
        for load in loads:
            load.wait()
        out_ref[...] = mlp_rows(x_ref[...], *kept)

    return pl.pallas_call(
        body,
        grid=(1,),
        out_shape=[jax.ShapeDtypeStruct(x.shape, F32)]
        + [pltpu.VMEM(w.shape[1:], BF16) for w in stacks],
        in_specs=[whole(x.shape)] + [pl.BlockSpec(memory_space=pl.ANY)] * 3,
        out_specs=[whole(x.shape)] + [pl.BlockSpec(memory_space=pltpu.VMEM)] * 3,
        scratch_shapes=[pltpu.SemaphoreType.DMA((3,))],
        compiler_params=params(12),
        cost_estimate=cost(6.0 * x.size * w_down.shape[1], 0),
        name="mlp_load",
    )(x, *[in_hbm(w) for w in stacks])


def mlp_kept(x, weights):
    def body(x_ref, wg_ref, wu_ref, wd_ref, out_ref):
        out_ref[...] = mlp_rows(x_ref[...], wg_ref, wu_ref, wd_ref).astype(BF16)

    return pl.pallas_call(
        body,
        grid=(1,),
        out_shape=jax.ShapeDtypeStruct(x.shape, BF16),
        in_specs=[whole(x.shape)] + [pl.BlockSpec(memory_space=pltpu.VMEM)] * 3,
        out_specs=whole(x.shape),
        compiler_params=params(12),
        cost_estimate=cost(6.0 * x.size * weights[2].shape[0], 0),
        name="mlp_kept",
    )(x, *[pltpu.with_memory_space_constraint(w, pltpu.VMEM) for w in weights])


def last_norm(h, parts, gain):
    def body(h_ref, *refs):
        gain_ref, out_ref = refs[-2:]
        value = add_parts(h_ref[...], refs[:-2])
        out_ref[...] = norm_rows(value, gain_ref[...]).astype(BF16)

    args = [h] + parts + [gain]
    return pl.pallas_call(
        body,
        grid=(1,),
        out_shape=jax.ShapeDtypeStruct(h.shape, BF16),
        in_specs=[whole(x.shape) for x in args],
        out_specs=whole(h.shape),
        compiler_params=params(8),
        name="last_norm",
    )(*args)


def head_stats(rows, wanted, bases, shards):
    count = sum(x.shape[0] for x in rows)
    width = rows[0].shape[1]
    cols = shards[0].shape[1]
    tile = next(t for t in (1024, 768, 512, 384, 256, 128) if cols % t == 0)
    chunk = tile // 2 if tile % 256 == 0 else tile
    per = cols // tile
    steps = per * len(shards)

    def body(base_ref, want_ref, *rest):
        given = rest[: len(rows)]
        w_refs = rest[len(rows) : len(rows) + len(shards)]
        out_ref, top, total, picked, wide, x_ref = rest[len(rows) + len(shards) :]
        step = pl.program_id(0)

        @pl.when(step == 0)
        def _():
            top[...] = jnp.full_like(top, NEG)
            total[...] = jnp.zeros_like(total)
            picked[...] = jnp.zeros_like(picked)
            wide[...] = jnp.broadcast_to(want_ref[...], wide.shape)
            at = 0
            for ref in given:
                x_ref[at : at + ref.shape[0]] = ref[...]
                at += ref.shape[0]

        lane = lax.broadcasted_iota(jnp.int32, (1, LANES), 1)

        def use(w_ref, index):
            start = base_ref[index] + (step - index * per) * tile
            local = wide[...]
            for at in range(0, tile, chunk):
                logits = dot(x_ref[...], w_ref[:, at : at + chunk])
                parts = [logits[:, c : c + LANES] for c in range(0, chunk, LANES)]
                best = parts[0]
                for part in parts[1:]:
                    best = jnp.maximum(best, part)
                old = top[...]
                best = jnp.maximum(best, old)
                acc = total[...] * jnp.exp(old - best)
                pick = picked[...]
                for n, part in enumerate(parts):
                    acc = acc + jnp.exp(part - best)
                    pick = pick + jnp.where(local == lane + (start + at + n * LANES), part, 0.0)
                top[...] = best
                total[...] = acc
                picked[...] = pick

        for index, w_ref in enumerate(w_refs):
            pl.when(step // per == index)(lambda r=w_ref, n=index: use(r, n))

        @pl.when(step == steps - 1)
        def _():
            best = jnp.max(top[...], axis=1, keepdims=True)
            acc = jnp.sum(total[...] * jnp.exp(top[...] - best), axis=1, keepdims=True)
            pick = jnp.sum(picked[...], axis=1, keepdims=True)
            packed = jnp.where(lane == 0, best, jnp.where(lane == 1, acc, pick))
            out_ref[...] = jnp.transpose(packed, (1, 0))[:8]

    def column_spec(index):
        return pl.BlockSpec((width, tile), lambda s: (0, jnp.clip(s - index * per, 0, per - 1)))

    return pl.pallas_call(
        body,
        grid=(steps,),
        out_shape=jax.ShapeDtypeStruct((8, count), F32),
        in_specs=[
            pl.BlockSpec(memory_space=pltpu.SMEM),
            whole(wanted.shape),
        ]
        + [whole(x.shape) for x in rows]
        + [column_spec(n) for n in range(len(shards))],
        out_specs=whole((8, count)),
        scratch_shapes=[pltpu.VMEM((count, LANES), F32)] * 3
        + [pltpu.VMEM((count, LANES), jnp.int32), pltpu.VMEM((count, width), BF16)],
        compiler_params=params(20),
        cost_estimate=cost(2.0 * count * width * cols * len(shards), 0),
        name="head_stats",
    )(bases, wanted, *rows, *[in_hbm(w) for w in shards])


def head_stats_mxu(rows, wanted, bases, shards):
    count = sum(x.shape[0] for x in rows)
    width = rows[0].shape[1]
    cols = shards[0].shape[1]
    deep, pair = 256, 512
    tile = 2 * pair
    per = cols // tile
    steps = per * len(shards)
    full, rest_k = width // deep, width % deep
    starts = [k * deep for k in range(full)] + ([width - deep] if rest_k else [])
    pieces = len(starts)
    piece = count // pieces
    padded = len(starts) * deep
    cuts = 7 if width % 112 == 0 else 1

    def body(base_ref, want_ref, *refs):
        given = refs[: len(rows)]
        sources = refs[len(rows) : len(rows) + len(shards)]
        out_ref, top, total, picked, wide, x_ref, w_buf, arrived = refs[len(rows) + len(shards) :]
        lane = lax.broadcasted_iota(jnp.int32, (1, LANES), 1)

        def copy_part(source, at, slot, n):
            part = pl.ds(n * (width // cuts), width // cuts)
            return pltpu.make_async_copy(
                source.at[part, pl.ds(at, tile)], w_buf.at[slot, part], arrived.at[slot, n]
            )

        def fetch(step):
            for index, source in enumerate(sources):

                @pl.when(step // per == index)
                def _(source=source, index=index):
                    at = pl.multiple_of((step - index * per) * tile, tile)
                    for n in range(cuts):
                        copy_part(source, at, step % 2, n).start()

        def column(step):
            start = base_ref[0] + step * tile
            for index in range(1, len(shards)):
                here = base_ref[index] + (step - index * per) * tile
                start = jnp.where(step >= index * per, here, start)
            return start

        def scoped(*accs):
            fetch(0)
            top[...] = jnp.full_like(top, NEG)
            total[...] = jnp.zeros_like(total)
            picked[...] = jnp.zeros_like(picked)
            wide[...] = jnp.broadcast_to(want_ref[...], wide.shape)
            at = 0
            for ref in given:
                size = ref.shape[0]
                x_ref[at : at + size, : full * deep] = ref[:, : full * deep]
                if rest_k:
                    blank = jnp.zeros((size, deep - rest_k), BF16)
                    x_ref[at : at + size, full * deep : padded - rest_k] = blank
                    x_ref[at : at + size, padded - rest_k :] = ref[:, full * deep :]
                at += size
            half = [[accs[(b * 2 + q) * pieces :][:pieces] for q in range(2)] for b in range(2)]

            def multiply(b, slot, k):
                for q in range(2):
                    at = b * pair + q * deep
                    register = k % 2
                    pltpu.matmul_push_rhs(
                        w_buf[slot, starts[k] : starts[k] + deep, at : at + deep],
                        staging_register=register,
                        mxu_index=q,
                    )
                    for n in range(pieces):
                        pltpu.matmul_acc_lhs(
                            half[b][q][n],
                            x_ref[n * piece : (n + 1) * piece, k * deep : (k + 1) * deep],
                            load_staged_rhs=register if n == 0 else None,
                        )

            def collect(b, n, start, fresh):
                at = slice(n * piece, (n + 1) * piece)
                parts = []
                for q in range(2):
                    found = pltpu.matmul_pop(half[b][q][n])
                    parts += [found[:, c : c + LANES] for c in range(0, deep, LANES)]
                best = parts[0]
                for part in parts[1:]:
                    best = jnp.maximum(best, part)
                old = top[at]
                best = jnp.maximum(best, old)
                acc = total[at] * jnp.exp(old - best)
                pick = picked[at]
                local = wide[at]
                for c, part in enumerate(parts):
                    acc = acc + jnp.exp(part - best)
                    pick = pick + jnp.where(local == lane + (start + c * LANES), part, 0.0)
                if fresh is not None:
                    best = jnp.where(fresh, NEG, best)
                    acc = jnp.where(fresh, 0.0, acc)
                    pick = jnp.where(fresh, 0.0, pick)
                top[at] = best
                total[at] = acc
                picked[at] = pick

            def step_fn(step, carry):
                slot = step % 2
                for n in range(cuts):
                    copy_part(sources[0], 0, slot, n).wait()
                pl.when(step + 1 < steps)(lambda: fetch(step + 1))
                before = column(jnp.maximum(step - 1, 0)) + pair
                start = column(step)
                for k in range(len(starts)):
                    multiply(0, slot, k)
                    collect(1, k, before, step == 0)
                for k in range(len(starts)):
                    multiply(1, slot, k)
                    collect(0, k, start, None)
                return carry

            lax.fori_loop(0, steps, step_fn, 0)
            for k in range(pieces):
                collect(1, k, column(steps - 1) + pair, None)
            best = jnp.max(top[...], axis=1, keepdims=True)
            acc = jnp.sum(total[...] * jnp.exp(top[...] - best), axis=1, keepdims=True)
            pick = jnp.sum(picked[...], axis=1, keepdims=True)
            packed = jnp.where(lane == 0, best, jnp.where(lane == 1, acc, pick))
            out_ref[...] = jnp.transpose(packed, (1, 0))[:8]

        kinds = [pltpu.ACC(q)((piece, deep), F32) for b in range(2) for q in range(2) for n in range(pieces)]
        pl.run_scoped(scoped, *kinds)

    return pl.pallas_call(
        body,
        grid=(1,),
        out_shape=jax.ShapeDtypeStruct((8, count), F32),
        in_specs=[
            pl.BlockSpec(memory_space=pltpu.SMEM),
            whole(wanted.shape),
        ]
        + [whole(x.shape) for x in rows]
        + [pl.BlockSpec(memory_space=pl.ANY)] * len(shards),
        out_specs=whole((8, count)),
        scratch_shapes=[pltpu.VMEM((count, LANES), F32)] * 3
        + [
            pltpu.VMEM((count, LANES), jnp.int32),
            pltpu.VMEM((count, padded), BF16),
            pltpu.VMEM((2, width, tile), BF16),
            pltpu.SemaphoreType.DMA((2, cuts)),
        ],
        compiler_params=params(20),
        cost_estimate=cost(2.0 * count * width * cols * len(shards), 0),
        name="head_stats_mxu",
    )(bases, wanted, *rows, *[in_hbm(w) for w in shards])


def shift(x, axes, distance, size, wrap):
    pairs = [(i, (i + distance) % size) for i in range(size) if wrap or i + distance < size]
    return lax.ppermute(x, axes, pairs)


def on_device(
    hidden_in,
    targets,
    doc_blocks,
    ref_milli,
    attn_gain,
    mlp_gain,
    final_gain,
    w_query,
    w_key,
    w_value,
    w_out,
    w_gate,
    w_up,
    w_down,
    w_head,
):
    zp_count = lax.axis_size("zp")
    core_count = lax.axis_size("core")
    dp_count = lax.axis_size(DP)
    tp_count = lax.axis_size("tensor")
    device_count = dp_count * tp_count
    row = lax.axis_index(DP)
    column = lax.axis_index("tensor")
    own_blocks, slice_len, width = hidden_in.shape
    block_len = slice_len * tp_count
    nblk = own_blocks * dp_count
    ndoc = doc_blocks.shape[0]
    tails = MAXB - 1
    own_count = own_blocks * slice_len
    vocab_shard = w_head.shape[1]

    direct = tp_count in (2, 4)

    def peer(x, k):
        return lax.ppermute(x, "tensor", [(i, i ^ k) for i in range(tp_count)])

    if core_count > 1:
        swap = [(i, core_count - 1 - i) for i in range(core_count)]
        shards = [w_head, lax.ppermute(w_head, "core", swap)]
        holders = [row, row - 2 * lax.axis_index("core") + 1]
    else:
        shards = [w_head]
        holders = [row]
    bases = jnp.stack([(r * tp_count + column) * vocab_shard for r in holders]).astype(jnp.int32)
    ids = targets.reshape(1, own_count)
    digits = jnp.concatenate([ids // 16384, ids // 128 % 128, ids % 128], axis=0).astype(BF16)
    digits = jnp.pad(digits, ((0, slice_len - 3), (0, 2 * w_key.shape[-1] - own_count)))

    owner, offset = doc_table(doc_blocks, nblk)
    own_ids = row * own_blocks + jnp.arange(own_blocks, dtype=jnp.int32)
    slot_doc, live = lookup(own_ids, owner, nblk)
    slot_off, unused = lookup(own_ids, offset, nblk)
    prior_ids = row * own_blocks - tails + jnp.arange(tails, dtype=jnp.int32)
    prior_doc, prior_inside = lookup(prior_ids, owner, nblk)
    key_doc = jnp.concatenate([jnp.where(prior_inside, prior_doc, -1), slot_doc])
    window_doc = jnp.stack([key_doc[i : i + MAXB] for i in range(own_blocks)])
    same = (window_doc == slot_doc[:, None]) & (window_doc >= 0)
    place = column * slice_len + jnp.arange(slice_len, dtype=jnp.int32)
    inner = jnp.arange(block_len, dtype=jnp.int32)
    causal = inner[None, :] <= place[:, None]
    slot = jnp.arange(MAXB, dtype=jnp.int32)
    seen = (slot[None, :, None] < tails) | causal[:, None, :]
    bias = jnp.where(same[:, None, :, None] & seen[None], 0.0, NEG).astype(F32)
    bias = bias.reshape(own_blocks, slice_len, MAXB * block_len)

    pos = (slot_off[:, None] * block_len + place[None, :]).reshape(-1).astype(F32)
    half = HEAD_DIM // 2
    lane = jnp.arange(LANES, dtype=jnp.int32)
    freq = jnp.exp((lane % half).astype(F32) * (-2.0 * math.log(1000000.0) / HEAD_DIM))
    angle = pos[:, None] * freq[None, :]
    cosine = jnp.cos(angle)
    sine = jnp.sin(angle) * jnp.where(lane % HEAD_DIM < half, -1.0, 1.0)[None, :]

    h = hidden_in.reshape(own_count, width)
    attn_gain = tall(attn_gain)
    mlp_gain = tall(mlp_gain)
    w_gate = w_gate.transpose(0, 2, 1)
    w_up = w_up.transpose(0, 2, 1)
    parts = []
    for layer in range(w_query.shape[0]):
        h, a, kv = key_value(h, parts, attn_gain, w_key, w_value, cosine, sine, layer)
        kvw = kv.shape[1]
        kv = kv.reshape(own_blocks, slice_len, kvw)
        tail = shift(kv[own_blocks - tails :], DP, 1, dp_count, False)
        q = queries(a, w_query, cosine, sine, layer)
        kv = jnp.concatenate([tail, kv] + ([digits[None]] if layer == 0 else []), axis=0)
        kv = lax.all_gather(kv, "tensor", axis=1, tiled=True)
        if layer == 0:
            found = kv[-1].reshape(tp_count, slice_len, kvw)[:, :3, :own_count].astype(jnp.int32)
            wanted_row = found[:, 0] * 16384 + found[:, 1] * 128 + found[:, 2]
            kv = kv[:-1]
        tail_pieces = [kv[:tails].reshape(-1, kvw)]
        own_pieces = [kv[tails:].reshape(-1, kvw)]
        h, b = attention(
            q,
            tail_pieces,
            own_pieces,
            bias,
            h,
            w_out,
            mlp_gain,
            layer,
        )
        if direct:
            given = [peer(b, k) for k in range(1, tp_count)]
            mine, *kept = mlp_load(b, w_gate, w_up, w_down, layer)
            parts = [mine]
            for k, x in enumerate(given, 1):
                parts.append(peer(mlp_kept(x, kept), k))
        else:
            flat = lax.all_gather(b, "tensor", axis=0, tiled=True)
            out = mlp(flat, w_gate, w_up, w_down, layer, BF16)
            out = out.reshape(tp_count, own_count, width)
            out = lax.all_to_all(out, "tensor", 0, 0, tiled=False)
            parts = [out[k] for k in range(tp_count)]
    final = last_norm(h, parts, tall(final_gain))

    zq_count = lax.axis_size("zq")
    turns = [(q, p) for p in range(zp_count) for q in range(zq_count)]

    def brought(x, turn):
        if turn == (0, 0):
            return x
        route = [
            (p * zq_count + q, (p + turn[1]) % zp_count * zq_count + (q + turn[0]) % zq_count)
            for p in range(zp_count)
            for q in range(zq_count)
        ]
        return lax.ppermute(x, ("zp", "zq"), route)

    def gathered(x):
        if direct:
            return [x] + [peer(x, k) for k in range(1, tp_count)]
        return [lax.all_gather(x, "tensor", axis=0, tiled=True)]

    if direct:
        order = [column ^ k for k in range(tp_count)]
        wanted_row = [lax.dynamic_slice_in_dim(wanted_row, k, 1, 0) for k in order]
        wanted_row = jnp.concatenate(wanted_row)
    wanted = [brought(wanted_row, turn).reshape(-1, 1) for turn in turns]
    chunk = gathered(final)
    done = chunk[-1]
    queue = [brought(final, turn) for turn in turns[1:3]]
    stats = []
    for n in range(len(turns)):
        following = None
        if n + 1 < len(turns):
            ahead, source, done = lax.optimization_barrier((queue.pop(0), final, done))
            following = gathered(ahead)
            if n + 3 < len(turns):
                queue.append(brought(source, turns[n + 3]))
        fits = vocab_shard % 1024 == 0 and sum(x.shape[0] for x in chunk) % 64 == 0
        stage = head_stats_mxu if fits else head_stats
        stats.append(stage(chunk, wanted[n], bases, shards))
        chunk = following
        bases, done = lax.optimization_barrier((bases, stats[-1]))
        stats[-1] = done
    stats = jnp.stack(stats)[:, :3].reshape(len(turns), 3, tp_count, own_count)
    stats = stats.transpose(0, 2, 1, 3).reshape(-1, 3, own_count)
    place_zp = jnp.arange(zp_count)[:, None, None]
    place_zq = jnp.arange(zq_count)[None, :, None]
    place_t = jnp.arange(tp_count)[None, None, :]
    at = (lax.axis_index("zp") - place_zp) % zp_count * zq_count
    at = (at + (lax.axis_index("zq") - place_zq) % zq_count) * tp_count
    at = at + (place_t ^ column if direct else place_t)
    stats = jnp.take(stats, at.reshape(-1), axis=0, mode="clip")
    stats = lax.all_to_all(stats, ("zp", "zq", "tensor"), 0, 0, tiled=False)
    peak = jnp.max(stats[:, 0], axis=0)
    total = jnp.sum(stats[:, 1] * jnp.exp(stats[:, 0] - peak[None]), axis=0)
    own_loss = jnp.log(total) + peak - jnp.sum(stats[:, 2], axis=0)
    own_loss = own_loss.reshape(own_blocks, slice_len)

    slot_sum = jnp.sum(own_loss, axis=1)
    hit = (slot_doc[:, None] == jnp.arange(ndoc, dtype=jnp.int32)[None, :]) & live[:, None]
    partial_docs = jnp.sum(jnp.where(hit, slot_sum[:, None], 0.0), axis=0)
    padded = jnp.pad(partial_docs, (0, LANES - ndoc))
    spread = jnp.broadcast_to(padded[None], (device_count, LANES))
    doc_total = jnp.sum(lax.all_to_all(spread, ALL, 0, 0, tiled=False), axis=0)[:ndoc]
    scores = ref_milli.astype(F32) * 0.001 - doc_total / (doc_blocks * block_len).astype(F32)
    return (own_loss, scores)


def solution(mesh):
    dp_count, tp_count = mesh.shape["dp"], mesh.shape["tensor"]
    core = 2 if dp_count % 2 == 0 else 1
    depth = dp_count // core
    pair = 2 if depth % 2 == 0 else 1
    devices = mesh.devices.reshape(depth // pair, pair, core, tp_count)
    return jax.shard_map(
        on_device,
        mesh=Mesh(devices, ALL),
        in_specs=(
            P(DP, "tensor", None),
            P(DP, "tensor"),
            P(),
            P(),
            P(),
            P(),
            P(),
            P(),
            P(),
            P(),
            P(),
            P(None, None, "tensor"),
            P(None, None, "tensor"),
            P(None, "tensor", None),
            P(None, ALL),
        ),
        out_specs=(P(DP, "tensor"), P()),
        check_vma=False,
    )
```
